256 devices in a mesh: lat: 8 (over x, core), lon: 32 (over y, z).
Axes of the slice: x: 4, y: 4, z: 8, core: 2. Of those that a mesh axis runs over, the one named last changes fastest.
Arguments:
- prediction_fields: float32 [4, 69, 1440, 1024], P(None, None, 'lon', 'lat'), may hold values from -16 to 16
- verifying_state: float32 [69, 1440, 1024], P(None, 'lon', 'lat'), may hold values from -16 to 16
- normal_state: float32 [69, 1440, 1024], P(None, 'lon', 'lat'), may hold values from -16 to 16
- evaluated_point_flag: int32 [1440, 1024], P('lon', 'lat'), may hold values 0 or 1
- parallels_each_strip: int32 [8], replicated, may hold values from 1 to 128, 721 in all
Outputs:
- parallel_quadratic_error: float32 [4, 69, 1024], P(None, None, 'lat')
- parallel_systematic_error: float32 [4, 69, 1024], P(None, None, 'lat')
- parallel_pattern_skill: float32 [4, 69, 1024], P(None, None, 'lat')
- rmse: float32 [4, 69], replicated
- systematic_error: float32 [4, 69], replicated
- pattern_skill: float32 [4, 69], replicated
The draws below stay inside these ranges and needn't reach their ends.
Inputs may be any that keep to these rules, and one draw needn't show every extreme that they name: `parallels_each_strip`: they sum to 721, and some band holds exactly 128 rows.
All inputs are finite; a program needn't handle non-finite values.
Results may differ from the reference program's by a relative error of at most 0.00002.
Values sent between devices are 32-bit elements.
A program may use at most 64 MiB of HBM per device.

```python
import math
import jax
import jax.numpy as jnp
import numpy as np
from jax import lax

VARS = 69
LEADS = 4
LAT_CAP = 128
LAT_BANDS = 8
NLAT = 721
EAST_WEST_SIZE = 1440
LAT_BUF = 1024


def common_fields(key):
    subkeys = jax.random.split(jax.random.fold_in(key, 4242), 8)
    climate = jax.random.normal(subkeys[0], (VARS, EAST_WEST_SIZE, LAT_BUF), jnp.float32)
    amplitude = jnp.exp(jax.random.uniform(subkeys[1], (VARS, 1, LAT_BUF), jnp.float32, jnp.log(0.5), jnp.log(2.0)))
    anomaly = jax.random.normal(subkeys[2], (VARS, EAST_WEST_SIZE, LAT_BUF), jnp.float32) * amplitude
    observed = climate + anomaly
    skill = jax.random.uniform(subkeys[4], (LEADS, VARS, 1, 1), jnp.float32, 0.3, 0.95)
    noise_scale = jax.random.uniform(subkeys[5], (LEADS, VARS, 1, 1), jnp.float32, 0.6, 1.2)
    drift = jax.random.uniform(subkeys[6], (LEADS, VARS, 1, LAT_BUF), jnp.float32, -0.6, 0.6)
    noise = jax.random.normal(subkeys[7], (LEADS, VARS, EAST_WEST_SIZE, LAT_BUF), jnp.float32)
    predicted = climate[None] + skill * anomaly[None] + noise_scale * amplitude[None] * noise + drift
    return (jnp.clip(predicted, -16.0, 16.0), jnp.clip(observed, -16.0, 16.0), jnp.clip(climate, -16.0, 16.0))


def draw_prediction_fields(key, part):
    return common_fields(key)[0]


def draw_verifying_state(key, part):
    return common_fields(key)[1]


def draw_normal_state(key, part):
    return common_fields(key)[2]


def place_ends(values, own_key, least, top_value):
    extent = values.shape
    index_at = [jax.random.randint(jax.random.fold_in(own_key, axis), (), 0, extent[axis]) for axis in range(len(extent))]
    values = values.at[tuple(index_at)].set(least)
    longest = extent.index(max(extent))
    index_at[longest] = (index_at[longest] + 1) % extent[longest]
    return values.at[tuple(index_at)].set(top_value)


def length_profile(count, total, limit, skew):
    portions = [(1 << 20) // math.isqrt(grade ** skew) + 1 for grade in range(2, count + 1)]
    spare, given = total - limit - (count - 1), [1] * (count - 1)
    while spare > 0:
        free = [i for i in range(count - 1) if given[i] < limit]
        mass, remaining = sum([portions[i] for i in free]), spare
        for i in free:
            extra = min(limit - given[i], max(1, remaining * portions[i] // mass), spare)
            given[i] = given[i] + extra
            spare = spare - extra
    return np.array([limit] + given)


def ragged(own_key, number_of, total, most, slope):
    if number_of == 2:
        one = jax.random.randint(own_key, (), max(1, total - most), min(most, total - 1) + 1)
        return jnp.stack([one, total - one])
    sizes = jnp.asarray(length_profile(number_of, total, most, slope), jnp.int32)
    twos = (number_of - 1) // 2
    donor, taker = sizes[1:1 + 2 * twos:2], sizes[2:2 + 2 * twos:2]
    margin = jnp.minimum(donor - 1, most - taker)
    passed = jax.random.randint(jax.random.fold_in(own_key, 1), (twos,), 0, 1 << 20) % (margin + 1)
    sizes = sizes.at[1:1 + 2 * twos:2].set(donor - passed).at[2:2 + 2 * twos:2].set(taker + passed)
    return sizes[jax.random.permutation(jax.random.fold_in(own_key, 2), number_of)]


def setup_inputs(seed: int = 0) -> dict:
    arg_keys = jax.random.split(jax.random.key(seed), 6)
    return {
        "prediction_fields": draw_prediction_fields(jax.random.fold_in(arg_keys[5], 71), 0),
        "verifying_state": draw_verifying_state(jax.random.fold_in(arg_keys[5], 71), 0),
        "normal_state": draw_normal_state(jax.random.fold_in(arg_keys[5], 71), 0),
        "evaluated_point_flag": place_ends((jax.random.randint(arg_keys[3], (EAST_WEST_SIZE, LAT_BUF), 0, 4) < 3).astype(jnp.int32), jax.random.fold_in(arg_keys[3], 1), 0, 1),
        "parallels_each_strip": ragged(arg_keys[4], LAT_BANDS, NLAT, LAT_CAP, 2).astype(jnp.int32),
    }


minimum_divisor = 0.1

def final_result(error_power_two, prediction_error, paired_anomaly_term, predicted_spread_sum, observed_dispersion, grid_point_tally):
    mean_square = error_power_two / grid_point_tally
    average_error = prediction_error / grid_point_tally
    covariance_sum = paired_anomaly_term / grid_point_tally / jnp.sqrt(jnp.maximum(predicted_spread_sum / grid_point_tally, minimum_divisor) * jnp.maximum(observed_dispersion / grid_point_tally, minimum_divisor))
    return (mean_square, average_error, covariance_sum)

def reference(prediction_fields, verifying_state, normal_state, evaluated_point_flag, parallels_each_strip):
    band_start = jnp.cumsum(parallels_each_strip) - parallels_each_strip
    slot_ids = jnp.arange(LAT_CAP, dtype=jnp.int32)
    global_row = (band_start[:, None] + slot_ids[None, :]).reshape(-1)
    inside_band = (slot_ids[None, :] < parallels_each_strip[:, None]).reshape(-1)
    angles = jnp.pi * jnp.arange(NLAT, dtype=jnp.float32) / (NLAT - 1)
    normalizer = jnp.sum(jnp.sin(angles))
    row_angle = jnp.pi * global_row.astype(jnp.float32) / (NLAT - 1)
    area_factors = jnp.where(inside_band, jnp.sin(row_angle) * NLAT / normalizer, 0.0).astype(jnp.float32)
    retain_filter = evaluated_point_flag.astype(jnp.float32) * inside_band.astype(jnp.float32)[None, :]
    observed_anomaly = verifying_state - normal_state
    observed_dispersion = lax.optimization_barrier(jnp.sum(retain_filter * observed_anomaly * observed_anomaly, axis=1))

    def by_horizon(predicted_step):
        predicted_anomaly = predicted_step - normal_state
        mistake_field = predicted_anomaly - observed_anomaly
        return (lax.optimization_barrier(jnp.sum(retain_filter * mistake_field * mistake_field, axis=1)), lax.optimization_barrier(jnp.sum(retain_filter * mistake_field, axis=1)), lax.optimization_barrier(jnp.sum(retain_filter * predicted_anomaly * observed_anomaly, axis=1)), lax.optimization_barrier(jnp.sum(retain_filter * predicted_anomaly * predicted_anomaly, axis=1)))
    error_power_two, prediction_error, paired_anomaly_term, predicted_spread_sum = lax.map(by_horizon, prediction_fields)
    parallel_quadratic_error, parallel_systematic_error, parallel_pattern_skill = final_result(error_power_two, prediction_error, paired_anomaly_term, predicted_spread_sum, observed_dispersion[None], EAST_WEST_SIZE)
    grid_points = NLAT * EAST_WEST_SIZE
    quadratic_error_total, systematic_error, pattern_skill = final_result(lax.optimization_barrier(jnp.sum(error_power_two * area_factors, axis=-1)), lax.optimization_barrier(jnp.sum(prediction_error * area_factors, axis=-1)), lax.optimization_barrier(jnp.sum(paired_anomaly_term * area_factors, axis=-1)), lax.optimization_barrier(jnp.sum(predicted_spread_sum * area_factors, axis=-1)), lax.optimization_barrier(jnp.sum(observed_dispersion * area_factors, axis=-1))[None], grid_points)
    rmse = jnp.sqrt(jnp.maximum(quadratic_error_total, minimum_divisor))
    return (parallel_quadratic_error, parallel_systematic_error, parallel_pattern_skill, rmse, systematic_error, pattern_skill)
```

```python
import functools
import math

import jax
import jax.numpy as jnp
from jax import lax
from jax.experimental import pallas as pl
from jax.experimental.pallas import tpu as pltpu
from jax.sharding import PartitionSpec as P

MESH = pl.DeviceIdType.MESH
Y, Z = 4, 8
LEADS, VARS = 4, 69
GV = 18
PAIRS = 9
ROWS = 4 * PAIRS + 3
SCORES = 3 * PAIRS
OFFS = (4, 3, 5, 2, 6, 1, 7, 0)
NLAT, NLON = 721, 1440
FLOOR = 0.1
SIN_SUM = sum(math.sin(math.pi * g / (NLAT - 1)) for g in range(NLAT))


def kernel(p, t, n, flag, bands, o0, o1, o2, g0, g1, g2,
           pbuf, tbuf, nbuf, kbuf, wbuf, part, rel, in_m, in_p, zin, sbuf, gath, lin, hall,
           isem, rel_s, rel_r, dir_s, fwd_s, m_r, p_r, z_s, z_r, a_s, a_r, ym_s, yp_s, ym_r, yp_r,
           opp_s, opp_r, l_s, l_r, h_s, h_r):
    lat, j = lax.axis_index("lat"), lax.axis_index("lon")
    nlat = 8
    y, z = j // Z, lax.rem(j, Z)
    up, down = lax.rem(y + 1, Y), lax.rem(y + Y - 1, Y)
    f32 = jnp.float32

    def at(yy, zz):
        return yy * Z + zz

    def zto(k):
        return lax.rem(z + OFFS[k], Z)

    def zfrom(k):
        return lax.rem(z + Z - OFFS[k], Z)

    def remote(src, dst, ss, rs, dev):
        return pltpu.make_async_remote_copy(
            src_ref=src, dst_ref=dst, send_sem=ss, recv_sem=rs, device_id=dev, device_id_type=MESH
        )

    def loads(r):
        base = jnp.minimum(GV * lax.rem(y + r, Y), VARS - GV)
        lons = pl.ds(0, 45)
        every = [
            pltpu.make_async_copy(n.at[pl.ds(base, GV)], nbuf.at[r, :, lons], isem.at[r, 0]),
            pltpu.make_async_copy(t.at[pl.ds(base, GV)], tbuf.at[r, :, lons], isem.at[r, 1]),
        ]
        for l in range(LEADS):
            every.append(
                pltpu.make_async_copy(p.at[l, pl.ds(base, GV)], pbuf.at[r, l, :, lons], isem.at[r, 2 + l])
            )
        return every

    order = (2, 1, 3, 0)
    for r in order:
        for c in loads(r):
            c.start()

    barrier = pltpu.get_barrier_semaphore()
    for d in range(1, Y * Z):
        pl.semaphore_signal(barrier, inc=1, device_id=(lat, lax.rem(j + d, Y * Z)), device_id_type=MESH)
    for d in range(1, nlat):
        pl.semaphore_signal(barrier, inc=1, device_id=(lax.rem(lat + d, nlat), j), device_id_type=MESH)

    part[...] = jnp.zeros_like(part)
    first, held = jnp.int32(0), jnp.int32(0)
    for b in range(nlat):
        first = first + jnp.where(b < lat, bands[b], 0)
        held = held + jnp.where(b == lat, bands[b], 0)
    lane = lax.broadcasted_iota(jnp.int32, (1, 128), 1)
    kbuf[40:48] = jnp.zeros((8, 128), jnp.int32)
    kbuf[0:45] = jnp.where(lane < held, flag[...], 0)
    angle = (first + lane).astype(f32) * (math.pi / (NLAT - 1))
    wbuf[...] = jnp.where(lane < held, jnp.sin(angle) * (NLAT / SIN_SUM), 0.0)

    def one(r, iv, b):
        square, offset, product, spread = ([None] * LEADS for _ in range(4))
        truth = None

        def add(total, x):
            return x if total is None else total + x

        for s in range(6):
            rows = pl.ds(8 * s, 8)
            m = kbuf[8 * s : 8 * s + 8] != 0
            nn = nbuf[r, b, rows, :]
            tt = jnp.where(m, tbuf[r, b, rows, :] - nn, 0.0)
            truth = add(truth, tt * tt)
            for l in range(LEADS):
                f = jnp.where(m, pbuf[r, l, b, rows, :] - nn, 0.0)
                e = f - tt
                square[l] = add(square[l], e * e)
                offset[l] = add(offset[l], e)
                product[l] = add(product[l], f * tt)
                spread[l] = add(spread[l], f * f)
        for l in range(LEADS):
            q = iv * LEADS + l
            zd = q // PAIRS
            i = q - zd * PAIRS
            for s, x in enumerate((square[l], offset[l], product[l], spread[l])):
                part[r, zd, pl.ds(s * PAIRS + i, 1), :] = jnp.sum(x, axis=0, keepdims=True)
        tr = jnp.sum(truth, axis=0, keepdims=True)
        for zd in ((iv * LEADS) // PAIRS, (iv * LEADS + LEADS - 1) // PAIRS):
            part[r, zd, pl.ds(4 * PAIRS + iv - (PAIRS * zd) // LEADS, 1), :] = tr

    def compute(r):
        off = GV * lax.rem(y + r, Y) - jnp.minimum(GV * lax.rem(y + r, Y), VARS - GV)
        for c in loads(r):
            c.wait()

        def step(c, carry):
            for u in range(3):
                iv = c * 3 + u
                one(r, iv, iv + off)
            return carry

        lax.fori_loop(0, (GV - off) // 3, step, 0)

    def to_relay(k):
        return remote(part.at[2, zto(k)], rel.at[k], rel_s.at[k], rel_r.at[k], (lat, at(up if k % 2 == 0 else down, z)))

    def direct(k):
        if k % 2:
            return remote(part.at[1, zto(k)], in_m.at[k], dir_s.at[k], m_r.at[k], (lat, at(up, z)))
        return remote(part.at[3, zto(k)], in_p.at[k], dir_s.at[k], p_r.at[k], (lat, at(down, z)))

    def relayed(k):
        if k % 2:
            return remote(part.at[3, zto(k)], in_p.at[k], fwd_s.at[k], p_r.at[k], (lat, at(down, z)))
        return remote(part.at[1, zto(k)], in_m.at[k], fwd_s.at[k], m_r.at[k], (lat, at(up, z)))

    def along_z(k):
        return remote(part.at[0, zto(k)], zin.at[k], z_s.at[k], z_r.at[k], (lat, at(y, zto(k))))

    compute(2)
    pl.semaphore_wait(barrier, Y * Z - 1 + nlat - 1)
    for k in range(Z):
        to_relay(k).start()
    compute(1)
    for k in range(1, Z, 2):
        direct(k).start()
    compute(3)
    for k in range(0, Z, 2):
        direct(k).start()
    compute(0)
    for k in range(Z):
        to_relay(k).wait_recv()
        r = 3 if k % 2 else 1
        part[r, zto(k)] = part[r, zto(k)] + rel[k]
        relayed(k).start()

    def from_y(k):
        a, b = (direct(k), relayed(k)) if k % 2 else (relayed(k), direct(k))
        a.wait_recv()
        b.wait_recv()
        return part[0, zto(k)] + (in_m[k] + in_p[k])

    for k in range(Z - 1):
        part[0, zto(k)] = from_y(k)
        along_z(k).start()
    s = from_y(Z - 1)
    for k in range(Z - 1):
        along_z(k).wait_recv()
        s = s + zin[k]

    c = 1.0 / NLON
    pair = lax.broadcasted_iota(jnp.int32, (PAIRS, 128), 0) + lax.rem(j, 4)
    sbuf[0:ROWS] = s
    square, offset = sbuf[0:9], sbuf[9:18]
    product, spread = sbuf[18:27], sbuf[27:36]
    truth = jnp.where(pair < 4, sbuf[36:37], jnp.where(pair < 8, sbuf[37:38], sbuf[38:39]))
    gath[j, 0:9] = square * c
    gath[j, 9:18] = offset * c
    gath[j, 18:27] = (product * c) / jnp.sqrt(jnp.maximum(spread * c, FLOOR) * jnp.maximum(truth * c, FLOOR))

    def spread_z(k, owner):
        return remote(gath.at[owner], gath.at[owner], a_s.at[k], a_r.at[k], (lat, at(y, zto(k))))

    def to_up(k, owner):
        return remote(gath.at[owner], gath.at[owner], ym_s.at[k], ym_r.at[k], (lat, at(up, z)))

    def to_down(k, owner):
        return remote(gath.at[owner], gath.at[owner], yp_s.at[k], yp_r.at[k], (lat, at(down, z)))

    def onward(k, owner):
        return remote(gath.at[owner], gath.at[owner], opp_s.at[k], opp_r.at[k], (lat, at(down if k % 2 else up, z)))

    for k in range(Z - 1):
        spread_z(k, j).start()
    to_up(Z - 1, j).start()
    to_down(Z - 1, j).start()

    sbuf[36:45] = truth
    sbuf[45:48] = jnp.zeros((3, 128), f32)
    column = jnp.sum(sbuf[...] * wbuf[...], axis=1, keepdims=True)
    here = lax.broadcasted_iota(jnp.int32, (48, 128), 0) == lax.broadcasted_iota(jnp.int32, (48, 128), 1)
    lin[lat] = jnp.sum(jnp.where(here, column, 0.0), axis=0, keepdims=True)

    def to_band(d):
        return remote(lin.at[lat], lin.at[lat], l_s.at[d], l_r.at[d], (lax.rem(lat + d, nlat), j))

    def from_band(d):
        src = lax.rem(lat + nlat - d, nlat)
        return remote(lin.at[src], lin.at[src], l_s.at[d], l_r.at[d], (lax.rem(lat + d, nlat), j))

    def to_all(d):
        return remote(hall.at[j], hall.at[j], h_s.at[d], h_r.at[d], (lat, lax.rem(j + d, Y * Z)))

    def from_all(d):
        src = lax.rem(j + Y * Z - d, Y * Z)
        return remote(hall.at[src], hall.at[src], h_s.at[d], h_r.at[d], (lat, lax.rem(j + d, Y * Z)))

    for d in range(1, nlat):
        to_band(d).start()
    for d in range(1, nlat):
        from_band(d).wait_recv()
    total = lin[0]
    for b in range(1, nlat):
        total = total + lin[b]
    total = total * (1.0 / (NLAT * NLON))
    over = pltpu.roll(total, 128 - 9, 1)
    under = pltpu.roll(total, 128 - 18, 1)
    skill = total / jnp.sqrt(jnp.maximum(over, FLOOR) * jnp.maximum(under, FLOOR))
    measures = jnp.where(lane < 9, jnp.sqrt(jnp.maximum(total, FLOOR)), jnp.where(lane < 18, total, skill))
    hall[j] = jnp.where(lane < SCORES, measures, 0.0)
    for d in range(1, Y * Z):
        to_all(d).start()

    for k in range(Z - 1):
        owner = at(y, zfrom(k))
        spread_z(k, owner).wait_recv()
        to_up(k, owner).start()
        to_down(k, owner).start()
    for k in (7, 0, 1, 2, 3, 4, 5, 6):
        below, above = at(down, zfrom(k)), at(up, zfrom(k))
        to_up(k, below).wait_recv()
        to_down(k, above).wait_recv()
        onward(k, above if k % 2 else below).start()
    opposite = lax.rem(y + 2, Y)
    for k in range(Z):
        onward(k, at(opposite, zfrom(k))).wait_recv()

    def place(c, pairs):
        for a in range(4):
            for i in range(PAIRS):
                q = a * PAIRS + i
                if q < pairs:
                    for m, o in enumerate((o0, o1, o2)):
                        o[q % LEADS, pl.ds(c * PAIRS + q // LEADS, 1), :] = gath[4 * c + a, m * PAIRS + i : m * PAIRS + i + 1]

    def placed(c, carry):
        place(c, 36)
        return carry

    lax.fori_loop(0, 7, placed, 0)
    place(7, LEADS * VARS - 7 * 36)

    for d in range(1, Y * Z):
        from_all(d).wait_recv()
    table = hall[:, 0, :]
    owner = lax.broadcasted_iota(jnp.int32, (Y * Z, 128), 0)
    var = lax.broadcasted_iota(jnp.int32, (Y * Z, 128), 1)
    for l in range(LEADS):
        q = var * LEADS + l
        mine = lax.shift_right_logical(q * 7282, 16)
        chosen = jnp.where(mine == owner, 1.0, 0.0)
        picked = lax.dot_general(
            table, chosen, (((0,), (0,)), ((), ())), precision=lax.Precision.HIGHEST, preferred_element_type=f32
        )[0:32]
        rest = q - mine * PAIRS
        for m, g in enumerate((g0, g1, g2)):
            line = jnp.sum(jnp.where(owner == rest + m * PAIRS, picked, 0.0), axis=0, keepdims=True)
            g[l : l + 1, :] = line[:, 0:VARS]

    for k in range(Z):
        to_relay(k).wait_send()
        direct(k).wait_send()
        relayed(k).wait_send()
        to_up(k, j).wait_send()
        to_down(k, j).wait_send()
        onward(k, j).wait_send()
    for k in range(Z - 1):
        along_z(k).wait_send()
        spread_z(k, j).wait_send()
    for d in range(1, nlat):
        to_band(d).wait_send()
    for d in range(1, Y * Z):
        to_all(d).wait_send()


def local(prediction_fields, verifying_state, normal_state, evaluated_point_flag, parallels_each_strip):
    f32 = jnp.float32
    hbm, vmem, smem = (pl.BlockSpec(memory_space=m) for m in (pltpu.HBM, pltpu.VMEM, pltpu.SMEM))
    dma = pltpu.SemaphoreType.DMA
    block = (Z, ROWS, 128)
    return pl.pallas_call(
        kernel,
        out_shape=[jax.ShapeDtypeStruct((LEADS, VARS, 128), f32)] * 3 + [jax.ShapeDtypeStruct((LEADS, VARS), f32)] * 3,
        in_specs=[hbm, hbm, hbm, vmem, smem],
        out_specs=[vmem] * 6,
        scratch_shapes=[
            pltpu.VMEM((Y, LEADS, GV, 48, 128), f32),
            pltpu.VMEM((Y, GV, 48, 128), f32),
            pltpu.VMEM((Y, GV, 48, 128), f32),
            pltpu.VMEM((48, 128), jnp.int32),
            pltpu.VMEM((1, 128), f32),
            pltpu.VMEM((Y, *block), f32),
            pltpu.VMEM(block, f32),
            pltpu.VMEM(block, f32),
            pltpu.VMEM(block, f32),
            pltpu.VMEM((Z - 1, ROWS, 128), f32),
            pltpu.VMEM((48, 128), f32),
            pltpu.VMEM((Y * Z, SCORES, 128), f32),
            pltpu.VMEM((8, 1, 128), f32),
            pltpu.VMEM((Y * Z, 1, 128), f32),
            dma((Y, 6)),
            *[dma((Z,))] * 16,
            *[dma((8,))] * 2,
            *[dma((Y * Z,))] * 2,
        ],
        compiler_params=pltpu.CompilerParams(
            collective_id=0, has_side_effects=True, vmem_limit_bytes=48 * 1024 * 1024
        ),
    )(prediction_fields, verifying_state, normal_state, evaluated_point_flag, parallels_each_strip)


def solution(mesh):
    placed = (P(None, None, "lon", "lat"), P(None, "lon", "lat"), P(None, "lon", "lat"), P("lon", "lat"), P())
    return jax.shard_map(
        local,
        mesh=mesh,
        in_specs=placed,
        out_specs=(P(None, None, "lat"), P(None, None, "lat"), P(None, None, "lat"), P(), P(), P()),
        check_vma=False,
    )
```

```python
import math

import jax
import jax.numpy as jnp
from jax import lax
from jax.experimental import pallas as pl
from jax.experimental.pallas import tpu as pltpu
from jax.sharding import PartitionSpec as P

MESH = pl.DeviceIdType.MESH
Y, Z = 4, 8
LEADS, VARS, LONS = 4, 69, 45
GV = 18
PAIRS = 9
PADDED = Y * Z * PAIRS
ROWS = 4 * PAIRS + 3
SCORES = 3 * PAIRS
TILES = 9
OFFS = (4, 3, 5, 2, 6, 1, 7, 0)
NLAT, NLON = 721, 1440
FLOOR = 0.1
SIN_SUM = sum(math.sin(math.pi * g / (NLAT - 1)) for g in range(NLAT))


def kernel(p, t, n, flag, bands, gath, g0, g1, g2,
           pbuf, tbuf, nbuf, kbuf, wbuf, part, ptru, rel, rel_t, in_m, in_mt, in_p, in_pt, tsum, zout, zin, sbuf, lin, hall,
           psem, tnsem, rel_s, rel_r, dir_s, fwd_s, m_r, p_r, z_s, z_r, a_s, a_r, ym_s, yp_s, ym_r, yp_r,
           opp_s, opp_r, l_s, l_r, h_s, h_r):
    lat, j = lax.axis_index("lat"), lax.axis_index("lon")
    nlat = 8
    y, z = j // Z, lax.rem(j, Z)
    up, down, opposite = (lax.rem(y + r, Y) for r in (1, Y - 1, 2))
    f32 = jnp.float32

    def at(yy, zz):
        return yy * Z + zz

    def zto(k):
        return lax.rem(z + OFFS[k], Z)

    def zfrom(k):
        return lax.rem(z + Z - OFFS[k], Z)

    def remote(src, dst, ss, rs, dev):
        return pltpu.make_async_remote_copy(
            src_ref=src, dst_ref=dst, send_sem=ss, recv_sem=rs, device_id=dev, device_id_type=MESH
        )

    def load_p(tile):
        return pltpu.make_async_copy(p.at[pl.ds(jnp.minimum(8 * tile, VARS - 8), 8)], pbuf.at[tile], psem.at[tile])

    def load_tn(c):
        lons, rows = pl.ds(9 * c, 9), pl.ds(0, VARS)
        return (
            pltpu.make_async_copy(n.at[lons], nbuf.at[lons, rows], tnsem.at[c, 0]),
            pltpu.make_async_copy(t.at[lons], tbuf.at[lons, rows], tnsem.at[c, 1]),
        )

    wrap_up, wrap_down = opposite == 0, opposite == Y - 1
    phases = (
        (2 * opposite, 3),
        (jnp.where(wrap_up, 6, 2 * opposite - 2), jnp.where(wrap_up, 3, 2)),
        (jnp.where(wrap_down, 0, 2 * opposite + 3), jnp.where(wrap_down, 3, 2)),
        (
            jnp.where(wrap_up, 5, jnp.where(opposite == 1, 7, jnp.where(opposite == 2, 0, 3))),
            jnp.where(wrap_up | wrap_down, 1, 2),
        ),
    )

    def start_p(phase):
        first, count = phases[phase]

        def go(i, carry):
            load_p(first + i).start()
            return carry

        lax.fori_loop(0, count, go, 0)

    for c in range(5):
        for d in load_tn(c):
            d.start()
        if c == 0:
            start_p(0)
    for phase in (1, 2, 3):
        start_p(phase)

    barrier = pltpu.get_barrier_semaphore()
    for d in range(1, Y * Z):
        pl.semaphore_signal(barrier, inc=1, device_id=(lat, lax.rem(j + d, Y * Z)), device_id_type=MESH)
    for d in range(1, nlat):
        pl.semaphore_signal(barrier, inc=1, device_id=(lax.rem(lat + d, nlat), j), device_id_type=MESH)

    part[:, LEADS * VARS : PADDED] = jnp.zeros((4, PADDED - LEADS * VARS, 128), f32)
    ptru[VARS : Y * GV] = jnp.zeros((Y * GV - VARS, 128), f32)
    first, held = jnp.int32(0), jnp.int32(0)
    for b in range(nlat):
        first = first + jnp.where(b < lat, bands[b], 0)
        held = held + jnp.where(b == lat, bands[b], 0)
    lane = lax.broadcasted_iota(jnp.int32, (1, 128), 1)
    for lon in range(LONS):
        kbuf[lon] = jnp.broadcast_to(jnp.where(lane < held, flag[lon : lon + 1], 0), (8, 128))
    angle = (first + lane).astype(f32) * (math.pi / (NLAT - 1))
    wbuf[...] = jnp.where(lane < held, jnp.sin(angle) * (NLAT / SIN_SUM), 0.0)

    prows = pbuf.reshape(TILES * 8 * LONS * LEADS, 128)

    def sums(tile):
        top = jnp.minimum(8 * tile, VARS - 8)
        base = tile * (8 * LONS * LEADS)

        def column(lon, totals):
            m = kbuf[lon] != 0
            nn = nbuf[lon, pl.ds(top, 8), :]
            tt = jnp.where(m, tbuf[lon, pl.ds(top, 8), :] - nn, 0.0)
            new = [totals[0] + tt * tt]
            for l in range(LEADS):
                square, offset, product, spread = totals[1 + 4 * l : 5 + 4 * l]
                f = jnp.where(m, prows[pl.ds(base + lon * LEADS + l, 8, stride=LONS * LEADS), :] - nn, 0.0)
                e = f - tt
                new += [square + e * e, offset + e, product + f * tt, spread + f * f]
            return tuple(new)

        def columns(c, totals):
            for u in range(9):
                totals = column(9 * c + u, totals)
            return totals

        totals = lax.fori_loop(0, 5, columns, (jnp.zeros((8, 128), f32),) * 17)
        ptru[pl.ds(top, 8), :] = totals[0]
        for l in range(LEADS):
            for s in range(4):
                part[s, pl.ds(top * LEADS + l, 8, stride=LEADS), :] = totals[1 + 4 * l + s]

    def compute(phase):
        first, count = phases[phase]

        def go(i, carry):
            load_p(first + i).wait()
            sums(first + i)
            return carry

        lax.fori_loop(0, count, go, 0)

    def block(g, k):
        return part.at[:, pl.ds(PAIRS * at(g, zto(k)), PAIRS), :]

    def group(g):
        return ptru.at[pl.ds(GV * g, GV), :]

    def take(g, k):
        return part[:, pl.ds(PAIRS * at(g, zto(k)), PAIRS), :]

    def to_relay(k):
        dev = (lat, at(down if k % 2 else up, z))
        if k == Z:
            return remote(group(opposite), rel_t, rel_s.at[k], rel_r.at[k], dev)
        return remote(block(opposite, k), rel.at[k], rel_s.at[k], rel_r.at[k], dev)

    def upwards(k, sems):
        dev = (lat, at(up, z))
        if k == Z:
            return remote(group(up), in_mt, sems.at[k], m_r.at[k], dev)
        return remote(block(up, k), in_m.at[k], sems.at[k], m_r.at[k], dev)

    def downwards(k, sems):
        dev = (lat, at(down, z))
        if k == Z:
            return remote(group(down), in_pt, sems.at[k], p_r.at[k], dev)
        return remote(block(down, k), in_p.at[k], sems.at[k], p_r.at[k], dev)

    def direct(k):
        return (upwards if k % 2 else downwards)(k, dir_s)

    def relayed(k):
        return (downwards if k % 2 else upwards)(k, fwd_s)

    def along_z(k):
        return remote(zout.at[k], zin.at[k], z_s.at[k], z_r.at[k], (lat, at(y, zto(k))))

    each = (Z, *range(Z))
    with jax.named_scope("load_tn"):
        for c in range(5):
            for d in load_tn(c):
                d.wait()
    with jax.named_scope("compute_a"):
        compute(0)
    with jax.named_scope("barrier"):
        pl.semaphore_wait(barrier, Y * Z - 1 + nlat - 1)
    for k in each:
        to_relay(k).start()
    with jax.named_scope("compute_b"):
        compute(1)
    for k in range(1, Z, 2):
        direct(k).start()
    with jax.named_scope("compute_c"):
        compute(2)
    for k in (Z, *range(0, Z, 2)):
        direct(k).start()
    with jax.named_scope("compute_d"):
        compute(3)
    for k in each:
        with jax.named_scope(f"relay#k={k}"):
            to_relay(k).wait_recv()
            g = down if k % 2 else up
            if k == Z:
                ptru[pl.ds(GV * g, GV), :] = ptru[pl.ds(GV * g, GV), :] + rel_t[...]
            else:
                part[:, pl.ds(PAIRS * at(g, zto(k)), PAIRS), :] = take(g, k) + rel[k]
            relayed(k).start()

    def arrived(k):
        upwards(k, dir_s if k % 2 else fwd_s).wait_recv()
        downwards(k, fwd_s if k % 2 else dir_s).wait_recv()

    arrived(Z)
    tsum[...] = ptru[pl.ds(GV * y, GV), :] + (in_mt[...] + in_pt[...])

    def summed(k, out):
        arrived(k)
        x = take(y, k) + (in_m[k] + in_p[k])
        for s in range(4):
            out[PAIRS * s : PAIRS * (s + 1)] = x[s]
        out[4 * PAIRS : ROWS] = tsum[pl.ds((PAIRS * zto(k)) // LEADS, 3), :]

    for k in range(Z - 1):
        with jax.named_scope(f"sum_y#k={k}"):
            summed(k, zout.at[k])
            along_z(k).start()
    summed(Z - 1, sbuf)
    s = sbuf[0:ROWS]
    for k in range(Z - 1):
        with jax.named_scope(f"sum_z#k={k}"):
            along_z(k).wait_recv()
            s = s + zin[k]

    c = 1.0 / NLON
    pair = lax.broadcasted_iota(jnp.int32, (PAIRS, 128), 0) + lax.rem(j, 4)
    sbuf[0:ROWS] = s
    square, offset = sbuf[0:9], sbuf[9:18]
    product, spread = sbuf[18:27], sbuf[27:36]
    truth = jnp.where(pair < 4, sbuf[36:37], jnp.where(pair < 8, sbuf[37:38], sbuf[38:39]))
    mine = pl.ds(PAIRS * j, PAIRS)
    gath[0, mine, :] = square * c
    gath[1, mine, :] = offset * c
    gath[2, mine, :] = (product * c) / jnp.sqrt(jnp.maximum(spread * c, FLOOR) * jnp.maximum(truth * c, FLOOR))

    def scores(owner):
        return gath.at[:, pl.ds(PAIRS * owner, PAIRS), :]

    def spread_z(k, owner):
        return remote(scores(owner), scores(owner), a_s.at[k], a_r.at[k], (lat, at(y, zto(k))))

    def to_up(k, owner):
        return remote(scores(owner), scores(owner), ym_s.at[k], ym_r.at[k], (lat, at(up, z)))

    def to_down(k, owner):
        return remote(scores(owner), scores(owner), yp_s.at[k], yp_r.at[k], (lat, at(down, z)))

    def onward(k, owner):
        return remote(scores(owner), scores(owner), opp_s.at[k], opp_r.at[k], (lat, at(down if k % 2 else up, z)))

    for k in range(Z - 1):
        spread_z(k, j).start()
    to_up(Z - 1, j).start()
    to_down(Z - 1, j).start()

    sbuf[36:45] = truth
    sbuf[45:48] = jnp.zeros((3, 128), f32)
    column = jnp.sum(sbuf[...] * wbuf[...], axis=1, keepdims=True)
    here = lax.broadcasted_iota(jnp.int32, (48, 128), 0) == lax.broadcasted_iota(jnp.int32, (48, 128), 1)
    lin[lat] = jnp.sum(jnp.where(here, column, 0.0), axis=0, keepdims=True)

    def to_band(d):
        return remote(lin.at[lat], lin.at[lat], l_s.at[d], l_r.at[d], (lax.rem(lat + d, nlat), j))

    def from_band(d):
        src = lax.rem(lat + nlat - d, nlat)
        return remote(lin.at[src], lin.at[src], l_s.at[d], l_r.at[d], (lax.rem(lat + d, nlat), j))

    def to_all(d):
        return remote(hall.at[j], hall.at[j], h_s.at[d], h_r.at[d], (lat, lax.rem(j + d, Y * Z)))

    def from_all(d):
        src = lax.rem(j + Y * Z - d, Y * Z)
        return remote(hall.at[src], hall.at[src], h_s.at[d], h_r.at[d], (lat, lax.rem(j + d, Y * Z)))

    for d in range(1, nlat):
        to_band(d).start()
    with jax.named_scope("bands"):
        for d in range(1, nlat):
            from_band(d).wait_recv()
    total = lin[0]
    for b in range(1, nlat):
        total = total + lin[b]
    total = total * (1.0 / (NLAT * NLON))
    over = pltpu.roll(total, 128 - 9, 1)
    under = pltpu.roll(total, 128 - 18, 1)
    skill = total / jnp.sqrt(jnp.maximum(over, FLOOR) * jnp.maximum(under, FLOOR))
    measures = jnp.where(lane < 9, jnp.sqrt(jnp.maximum(total, FLOOR)), jnp.where(lane < 18, total, skill))
    hall[j] = jnp.where(lane < SCORES, measures, 0.0)
    for d in range(1, Y * Z):
        to_all(d).start()

    for k in range(Z - 1):
        with jax.named_scope(f"gather_z#k={k}"):
            owner = at(y, zfrom(k))
            spread_z(k, owner).wait_recv()
            to_up(k, owner).start()
            to_down(k, owner).start()
    for k in (7, 0, 1, 2, 3, 4, 5, 6):
        with jax.named_scope(f"gather_y#k={k}"):
            below, above = at(down, zfrom(k)), at(up, zfrom(k))
            to_up(k, below).wait_recv()
            to_down(k, above).wait_recv()
            onward(k, above if k % 2 else below).start()
    for k in range(Z):
        with jax.named_scope(f"gather_o#k={k}"):
            onward(k, at(opposite, zfrom(k))).wait_recv()

    with jax.named_scope("globals"):
        for d in range(1, Y * Z):
            from_all(d).wait_recv()
    table = hall[:, 0, :]
    owner = lax.broadcasted_iota(jnp.int32, (Y * Z, 128), 0)
    var = lax.broadcasted_iota(jnp.int32, (Y * Z, 128), 1)
    for l in range(LEADS):
        q = var * LEADS + l
        mine = lax.shift_right_logical(q * 7282, 16)
        chosen = jnp.where(mine == owner, 1.0, 0.0)
        picked = lax.dot_general(
            table, chosen, (((0,), (0,)), ((), ())), precision=lax.Precision.HIGHEST, preferred_element_type=f32
        )[0:32]
        rest = q - mine * PAIRS
        for m, g in enumerate((g0, g1, g2)):
            line = jnp.sum(jnp.where(owner == rest + m * PAIRS, picked, 0.0), axis=0, keepdims=True)
            g[l : l + 1, :] = line[:, 0:VARS]

    for k in each:
        to_relay(k).wait_send()
        direct(k).wait_send()
        relayed(k).wait_send()
    for k in range(Z):
        to_up(k, j).wait_send()
        to_down(k, j).wait_send()
        onward(k, j).wait_send()
    for k in range(Z - 1):
        along_z(k).wait_send()
        spread_z(k, j).wait_send()
    for d in range(1, nlat):
        to_band(d).wait_send()
    for d in range(1, Y * Z):
        to_all(d).wait_send()


def writer(gath, s0, s1, s2, o0, o1, o2, g0, g1, g2, sems):
    rows = LEADS * VARS
    copies = [
        pltpu.make_async_copy(gath.at[m, pl.ds(0, rows)], o.reshape(rows, 128), sems.at[m])
        for m, o in enumerate((o0, o1, o2))
    ]
    copies += [
        pltpu.make_async_copy(s, g, sems.at[3 + m]) for m, (s, g) in enumerate(((s0, g0), (s1, g1), (s2, g2)))
    ]
    for c in copies:
        c.start()
    for c in copies:
        c.wait()


def local(prediction_fields, verifying_state, normal_state, evaluated_point_flag, parallels_each_strip):
    f32 = jnp.float32
    hbm, vmem, smem = (pl.BlockSpec(memory_space=m) for m in (pltpu.HBM, pltpu.VMEM, pltpu.SMEM))
    dma = pltpu.SemaphoreType.DMA
    single = [jax.ShapeDtypeStruct((LEADS, VARS), f32)] * 3
    gathered, *means = pl.pallas_call(
        kernel,
        out_shape=[jax.ShapeDtypeStruct((3, PADDED, 128), f32)] + single,
        in_specs=[hbm, hbm, hbm, vmem, smem],
        out_specs=[vmem] * 4,
        scratch_shapes=[
            pltpu.VMEM((TILES, 8, LONS, LEADS, 128), f32),
            pltpu.VMEM((LONS, 72, 128), f32),
            pltpu.VMEM((LONS, 72, 128), f32),
            pltpu.VMEM((LONS, 8, 128), jnp.int32),
            pltpu.VMEM((1, 128), f32),
            pltpu.VMEM((4, PADDED, 128), f32),
            pltpu.VMEM((Y * GV, 128), f32),
            *[pltpu.VMEM((Z, 4, PAIRS, 128), f32), pltpu.VMEM((GV, 128), f32)] * 3,
            pltpu.VMEM((GV, 128), f32),
            pltpu.VMEM((Z - 1, ROWS, 128), f32),
            pltpu.VMEM((Z - 1, ROWS, 128), f32),
            pltpu.VMEM((48, 128), f32),
            pltpu.VMEM((8, 1, 128), f32),
            pltpu.VMEM((Y * Z, 1, 128), f32),
            dma((TILES,)),
            dma((5, 2)),
            *[dma((Z + 1,))] * 6,
            *[dma((Z,))] * 10,
            *[dma((8,))] * 2,
            *[dma((Y * Z,))] * 2,
        ],
        compiler_params=pltpu.CompilerParams(
            collective_id=0, has_side_effects=True, vmem_limit_bytes=53 * 1024 * 1024
        ),
    )(
        jnp.transpose(prediction_fields, (1, 2, 0, 3)),
        jnp.transpose(verifying_state, (1, 0, 2)),
        jnp.transpose(normal_state, (1, 0, 2)),
        evaluated_point_flag,
        parallels_each_strip,
    )
    *zonal, a, b, c = pl.pallas_call(
        writer,
        out_shape=[jax.ShapeDtypeStruct((VARS, LEADS, 128), f32)] * 3 + single,
        in_specs=[vmem] * 4,
        out_specs=[hbm] * 6,
        scratch_shapes=[dma((6,))],
        compiler_params=pltpu.CompilerParams(vmem_limit_bytes=2 * 1024 * 1024),
    )(gathered, *means)
    return (*(jnp.transpose(o, (1, 0, 2)) for o in zonal), a, b, c)


def solution(mesh):
    placed = (P(None, None, "lon", "lat"), P(None, "lon", "lat"), P(None, "lon", "lat"), P("lon", "lat"), P())
    return jax.shard_map(
        local,
        mesh=mesh,
        in_specs=placed,
        out_specs=(P(None, None, "lat"), P(None, None, "lat"), P(None, None, "lat"), P(), P(), P()),
        check_vma=False,
    )
```

```python
import math

import jax
import jax.numpy as jnp
from jax import lax
from jax.experimental import pallas as pl
from jax.experimental.pallas import tpu as pltpu
from jax.sharding import PartitionSpec as P

MESH = pl.DeviceIdType.MESH
Y, Z = 4, 8
LEADS, VARS, LONS = 4, 69, 45
GV = 18
PAIRS = 9
PADDED = Y * Z * PAIRS
ROWS = 4 * PAIRS + 3
SCORES = 3 * PAIRS
TILES = 9
OFFS = (4, 3, 5, 2, 6, 1, 7, 0)
NLAT, NLON = 721, 1440
FLOOR = 0.1
SIN_SUM = sum(math.sin(math.pi * g / (NLAT - 1)) for g in range(NLAT))


def kernel(p, t, n, flag, bands, gath, g0, g1, g2,
           pbuf, tnbuf, fbuf, brow, kbuf, wbuf, part, ptru, rel, rel_t, in_m, in_mt, in_p, in_pt, tsum, zout, zin, sbuf,
           lin, hall, lsem, fsem, rel_r, fwd_r, a_r, y_r, sent, got):
    lat, j = lax.axis_index("lat"), lax.axis_index("lon")
    nlat = 8
    y, z = j // Z, lax.rem(j, Z)
    up, down, opposite = (lax.rem(y + r, Y) for r in (1, Y - 1, 2))
    f32 = jnp.float32

    def at(yy, zz):
        return yy * Z + zz

    def zto(k):
        return lax.rem(z + OFFS[k], Z)

    def zfrom(k):
        return lax.rem(z + Z - OFFS[k], Z)

    def remote(src, dst, ss, rs, dev):
        return pltpu.make_async_remote_copy(
            src_ref=src, dst_ref=dst, send_sem=ss, recv_sem=rs, device_id=dev, device_id_type=MESH
        )

    def started(ref, sem):
        return pltpu.make_async_copy(ref, ref, sem)

    def load(tile):
        v = pl.ds(jnp.minimum(8 * tile, VARS - 8), 8)
        pltpu.make_async_copy(n.at[:, v], tnbuf.at[tile, 0], lsem.at[0, tile]).start()
        pltpu.make_async_copy(t.at[:, v], tnbuf.at[tile, 1], lsem.at[0, tile]).start()
        pltpu.make_async_copy(p.at[v], pbuf.at[tile], lsem.at[1, tile]).start()

    wrap_up, wrap_down = opposite == 0, opposite == Y - 1
    phases = (
        (2 * opposite, 3),
        (jnp.where(wrap_up, 6, 2 * opposite - 2), jnp.where(wrap_up, 3, 2)),
        (jnp.where(wrap_down, 0, 2 * opposite + 3), jnp.where(wrap_down, 3, 2)),
        (
            jnp.where(wrap_up, 5, jnp.where(opposite == 1, 7, jnp.where(opposite == 2, 0, 3))),
            jnp.where(wrap_up | wrap_down, 1, 2),
        ),
    )

    barrier = pltpu.get_barrier_semaphore()
    for d in range(1, nlat):
        pl.semaphore_signal(barrier, inc=1, device_id=(lax.rem(lat + d, nlat), j), device_id_type=MESH)
    for d in range(1, Y * Z):
        pl.semaphore_signal(barrier, inc=1, device_id=(lat, lax.rem(j + d, Y * Z)), device_id_type=MESH)

    def start_loads(phase):
        first, count = phases[phase]

        def go(i, carry):
            load(first + i)
            return carry

        lax.fori_loop(0, count, go, 0)

    small = (pltpu.make_async_copy(flag, fbuf, fsem.at[0]), pltpu.make_async_copy(bands, brow, fsem.at[1]))
    for d in small:
        d.start()
    for phase in range(4):
        start_loads(phase)

    part[:, LEADS * VARS : PADDED] = jnp.zeros((4, PADDED - LEADS * VARS, 128), f32)
    ptru[VARS : Y * GV] = jnp.zeros((Y * GV - VARS, 128), f32)
    for d in small:
        d.wait()
    first, held = jnp.int32(0), jnp.int32(0)
    for b in range(nlat):
        first = first + jnp.where(b < lat, brow[b], 0)
        held = held + jnp.where(b == lat, brow[b], 0)
    lane = lax.broadcasted_iota(jnp.int32, (1, 128), 1)
    for lon in range(LONS):
        kbuf[lon] = jnp.broadcast_to(jnp.where(lane < held, fbuf[lon : lon + 1], 0), (8, 128))
    angle = (first + lane).astype(f32) * (math.pi / (NLAT - 1))
    wbuf[...] = jnp.where(lane < held, jnp.sin(angle) * (NLAT / SIN_SUM), 0.0)

    prows = pbuf.reshape(TILES * 8 * LONS * LEADS, 128)

    def sums(tile):
        top = jnp.minimum(8 * tile, VARS - 8)
        base = tile * (8 * LONS * LEADS)

        def column(lon, totals):
            m = kbuf[lon] != 0
            nn = tnbuf[tile, 0, lon]
            tt = jnp.where(m, tnbuf[tile, 1, lon] - nn, 0.0)
            new = [totals[0] + tt * tt]
            for l in range(LEADS):
                square, offset, product, spread = totals[1 + 4 * l : 5 + 4 * l]
                f = jnp.where(m, prows[pl.ds(base + lon * LEADS + l, 8, stride=LONS * LEADS), :] - nn, 0.0)
                e = f - tt
                new += [square + e * e, offset + e, product + f * tt, spread + f * f]
            return tuple(new)

        def columns(c, totals):
            for u in range(9):
                totals = column(9 * c + u, totals)
            return totals

        totals = lax.fori_loop(0, 5, columns, (jnp.zeros((8, 128), f32),) * 17)
        ptru[pl.ds(top, 8), :] = totals[0]
        for l in range(LEADS):
            for s in range(4):
                part[s, pl.ds(top * LEADS + l, 8, stride=LEADS), :] = totals[1 + 4 * l + s]

    def compute(phase):
        first, count = phases[phase]

        def go(i, carry):
            started(tnbuf.at[first + i], lsem.at[0, first + i]).wait()
            started(pbuf.at[first + i], lsem.at[1, first + i]).wait()
            sums(first + i)
            return carry

        lax.fori_loop(0, count, go, 0)

    def block(g, k):
        return part.at[:, pl.ds(PAIRS * at(g, zto(k)), PAIRS), :]

    def group(g):
        return ptru.at[pl.ds(GV * g, GV), :]

    def take(g, k):
        return part[:, pl.ds(PAIRS * at(g, zto(k)), PAIRS), :]

    REL, DIR, FWD, TRU, ZS, AS, UPS, DOWNS, OPPS, LS, HS = range(11)
    Z_R, DIR_UP, DIR_DOWN, OPP_R, L_R, H_R, TRU_DOWN = range(7)

    def to_relay(k):
        dev = (lat, at(down if k % 2 else up, z))
        if k == Z:
            return remote(group(opposite), rel_t, sent.at[TRU], rel_r.at[k], dev)
        return remote(block(opposite, k), rel.at[k], sent.at[REL], rel_r.at[k], dev)

    def direct(k):
        if k == Z:
            return remote(group(down), in_pt, sent.at[TRU], got.at[TRU_DOWN], (lat, at(down, z)))
        if k % 2:
            return remote(block(up, k), in_m.at[k], sent.at[DIR], got.at[DIR_UP], (lat, at(up, z)))
        return remote(block(down, k), in_p.at[k], sent.at[DIR], got.at[DIR_DOWN], (lat, at(down, z)))

    def relayed(k):
        if k == Z:
            return remote(group(up), in_mt, sent.at[TRU], fwd_r.at[k], (lat, at(up, z)))
        if k % 2:
            return remote(block(down, k), in_p.at[k], sent.at[FWD], fwd_r.at[k], (lat, at(down, z)))
        return remote(block(up, k), in_m.at[k], sent.at[FWD], fwd_r.at[k], (lat, at(up, z)))

    def along_z(k):
        return remote(zout.at[k], zin.at[k], sent.at[ZS], got.at[Z_R], (lat, at(y, zto(k))))

    each = (Z, *range(Z))
    with jax.named_scope("compute_a"):
        compute(0)
    with jax.named_scope("barrier"):
        pl.semaphore_wait(barrier, Y * Z - 1 + nlat - 1)
    for k in each:
        to_relay(k).start()
    with jax.named_scope("compute_b"):
        compute(1)
    for k in range(1, Z, 2):
        direct(k).start()
    with jax.named_scope("compute_c"):
        compute(2)
    for k in (Z, *range(0, Z, 2)):
        direct(k).start()
    with jax.named_scope("compute_d"):
        compute(3)
    for k in each:
        with jax.named_scope(f"relay#k={k}"):
            to_relay(k).wait_recv()
            g = down if k % 2 else up
            if k == Z:
                ptru[pl.ds(GV * g, GV), :] = ptru[pl.ds(GV * g, GV), :] + rel_t[...]
            else:
                part[:, pl.ds(PAIRS * at(g, zto(k)), PAIRS), :] = take(g, k) + rel[k]
            relayed(k).start()

    direct(Z).wait_recv()
    relayed(Z).wait_recv()
    started(in_m.at[0:4], got.at[DIR_UP]).wait()
    started(in_p.at[0:4], got.at[DIR_DOWN]).wait()
    tsum[...] = ptru[pl.ds(GV * y, GV), :] + (in_mt[...] + in_pt[...])

    def summed(k, out):
        relayed(k).wait_recv()
        x = take(y, k) + (in_m[k] + in_p[k])
        for s in range(4):
            out[PAIRS * s : PAIRS * (s + 1)] = x[s]
        out[4 * PAIRS : ROWS] = tsum[pl.ds((PAIRS * zto(k)) // LEADS, 3), :]

    for k in range(Z - 1):
        with jax.named_scope(f"sum_y#k={k}"):
            summed(k, zout.at[k])
            along_z(k).start()
    summed(Z - 1, sbuf)
    s = sbuf[0:ROWS]
    with jax.named_scope("sum_z"):
        started(zin, got.at[Z_R]).wait()
    for k in range(Z - 1):
        s = s + zin[k]

    c = 1.0 / NLON
    pair = lax.broadcasted_iota(jnp.int32, (PAIRS, 128), 0) + lax.rem(j, 4)
    sbuf[0:ROWS] = s
    square, offset = sbuf[0:9], sbuf[9:18]
    product, spread = sbuf[18:27], sbuf[27:36]
    truth = jnp.where(pair < 4, sbuf[36:37], jnp.where(pair < 8, sbuf[37:38], sbuf[38:39]))
    mine = pl.ds(PAIRS * j, PAIRS)
    gath[0, mine, :] = square * c
    gath[1, mine, :] = offset * c
    gath[2, mine, :] = (product * c) / jnp.sqrt(jnp.maximum(spread * c, FLOOR) * jnp.maximum(truth * c, FLOOR))

    def scores(owner):
        return gath.at[:, pl.ds(PAIRS * owner, PAIRS), :]

    def spread_z(k, owner):
        return remote(scores(owner), scores(owner), sent.at[AS], a_r.at[k], (lat, at(y, zto(k))))

    def to_up(k, owner):
        return remote(scores(owner), scores(owner), sent.at[UPS], y_r.at[k], (lat, at(up, z)))

    def to_down(k, owner):
        return remote(scores(owner), scores(owner), sent.at[DOWNS], y_r.at[k], (lat, at(down, z)))

    def onward(k, owner):
        return remote(scores(owner), scores(owner), sent.at[OPPS], got.at[OPP_R], (lat, at(down if k % 2 else up, z)))

    for k in range(Z - 1):
        spread_z(k, j).start()
    to_up(Z - 1, j).start()
    to_down(Z - 1, j).start()

    sbuf[36:45] = truth
    sbuf[45:48] = jnp.zeros((3, 128), f32)
    column = jnp.sum(sbuf[...] * wbuf[...], axis=1, keepdims=True)
    here = lax.broadcasted_iota(jnp.int32, (48, 128), 0) == lax.broadcasted_iota(jnp.int32, (48, 128), 1)
    lin[lat] = jnp.sum(jnp.where(here, column, 0.0), axis=0, keepdims=True)

    def to_band(d):
        return remote(lin.at[lat], lin.at[lat], sent.at[LS], got.at[L_R], (lax.rem(lat + d, nlat), j))

    def to_all(d):
        return remote(hall.at[j], hall.at[j], sent.at[HS], got.at[H_R], (lat, lax.rem(j + d, Y * Z)))

    for d in range(1, nlat):
        to_band(d).start()
    def from_z(k):
        with jax.named_scope(f"gather_z#k={k}"):
            owner = at(y, zfrom(k))
            spread_z(k, owner).wait_recv()
            to_up(k, owner).start()
            to_down(k, owner).start()

    def from_y(k):
        with jax.named_scope(f"gather_y#k={k}"):
            below, above = at(down, zfrom(k)), at(up, zfrom(k))
            started(gath.at[0, 0 : 2 * SCORES], y_r.at[k]).wait()
            onward(k, above if k % 2 else below).start()

    near = (5, 6, 3, 4, 1, 2, 0)
    for k in near[:2]:
        from_z(k)
    from_y(Z - 1)
    for k in near[2:]:
        from_z(k)
    with jax.named_scope("bands"):
        started(lin.at[0 : nlat - 1], got.at[L_R]).wait()
    total = lin[0]
    for b in range(1, nlat):
        total = total + lin[b]
    total = total * (1.0 / (NLAT * NLON))
    over = pltpu.roll(total, 128 - 9, 1)
    under = pltpu.roll(total, 128 - 18, 1)
    skill = total / jnp.sqrt(jnp.maximum(over, FLOOR) * jnp.maximum(under, FLOOR))
    measures = jnp.where(lane < 9, jnp.sqrt(jnp.maximum(total, FLOOR)), jnp.where(lane < 18, total, skill))
    hall[j] = jnp.where(lane < SCORES, measures, 0.0)
    for d in range(1, Y * Z):
        to_all(d).start()

    for k in near:
        from_y(k)
    with jax.named_scope("globals"):
        started(hall.at[0 : Y * Z - 1], got.at[H_R]).wait()
    table = hall[:, 0, :]
    owner = lax.broadcasted_iota(jnp.int32, (Y * Z, 128), 0)
    var = lax.broadcasted_iota(jnp.int32, (Y * Z, 128), 1)
    chosen = []
    for l in range(LEADS):
        mine = lax.shift_right_logical((var * LEADS + l) * 7282, 16)
        chosen.append(jnp.where(mine == owner, 1.0, 0.0))
    every = lax.dot_general(
        table,
        jnp.concatenate(chosen, axis=1),
        (((0,), (0,)), ((), ())),
        precision=lax.Precision.HIGHEST,
        preferred_element_type=f32,
    )
    for l in range(LEADS):
        q = var * LEADS + l
        picked = every[0 : Y * Z, 128 * l : 128 * (l + 1)]
        rest = q - lax.shift_right_logical(q * 7282, 16) * PAIRS
        for m, g in enumerate((g0, g1, g2)):
            line = jnp.sum(jnp.where(owner == rest + m * PAIRS, picked, 0.0), axis=0, keepdims=True)
            g[l : l + 1, :] = line[:, 0:VARS]

    with jax.named_scope("gather_o"):
        started(gath.at[0, 0 : Z * SCORES], got.at[OPP_R]).wait()

    with jax.named_scope("sends"):
        for i, ref in (
            (REL, rel),
            (DIR, rel),
            (FWD, rel),
            (TRU, ptru.at[0 : 3 * GV]),
            (ZS, zin),
            (AS, gath.at[0, 0 : (Z - 1) * SCORES]),
            (UPS, gath.at[0, 0 : Z * SCORES]),
            (DOWNS, gath.at[0, 0 : Z * SCORES]),
            (OPPS, gath.at[0, 0 : Z * SCORES]),
            (LS, hall.at[0 : nlat - 1]),
            (HS, hall.at[0 : Y * Z - 1]),
        ):
            started(ref, sent.at[i]).wait()


def writer(gath, s0, s1, s2, o0, o1, o2, g0, g1, g2, sems):
    rows = LEADS * VARS
    copies = [
        pltpu.make_async_copy(gath.at[m, pl.ds(0, rows)], o.reshape(rows, 128), sems.at[m])
        for m, o in enumerate((o0, o1, o2))
    ]
    copies += [
        pltpu.make_async_copy(s, g, sems.at[3 + m]) for m, (s, g) in enumerate(((s0, g0), (s1, g1), (s2, g2)))
    ]
    for c in copies:
        c.start()
    for c in copies:
        c.wait()


def local(prediction_fields, verifying_state, normal_state, evaluated_point_flag, parallels_each_strip):
    f32 = jnp.float32
    hbm, vmem = pl.BlockSpec(memory_space=pltpu.HBM), pl.BlockSpec(memory_space=pltpu.VMEM)
    dma = pltpu.SemaphoreType.DMA
    single = [jax.ShapeDtypeStruct((LEADS, VARS), f32)] * 3
    gathered, *means = pl.pallas_call(
        kernel,
        out_shape=[jax.ShapeDtypeStruct((3, PADDED, 128), f32)] + single,
        in_specs=[hbm] * 5,
        out_specs=[vmem] * 4,
        scratch_shapes=[
            pltpu.VMEM((TILES, 8, LONS, LEADS, 128), f32),
            pltpu.VMEM((TILES, 2, LONS, 8, 128), f32),
            pltpu.VMEM((LONS, 128), jnp.int32),
            pltpu.SMEM((8,), jnp.int32),
            pltpu.VMEM((LONS, 8, 128), jnp.int32),
            pltpu.VMEM((1, 128), f32),
            pltpu.VMEM((4, PADDED, 128), f32),
            pltpu.VMEM((Y * GV, 128), f32),
            *[pltpu.VMEM((Z, 4, PAIRS, 128), f32), pltpu.VMEM((GV, 128), f32)] * 3,
            pltpu.VMEM((GV, 128), f32),
            pltpu.VMEM((Z - 1, ROWS, 128), f32),
            pltpu.VMEM((Z - 1, ROWS, 128), f32),
            pltpu.VMEM((48, 128), f32),
            pltpu.VMEM((8, 1, 128), f32),
            pltpu.VMEM((Y * Z, 1, 128), f32),
            dma((2, TILES)),
            dma((2,)),
            *[dma((Z + 1,))] * 2,
            dma((Z - 1,)),
            dma((Z,)),
            dma((11,)),
            dma((7,)),
        ],
        compiler_params=pltpu.CompilerParams(
            collective_id=0, has_side_effects=True, vmem_limit_bytes=32 * 1024 * 1024
        ),
    )(
        *(
            pltpu.with_memory_space_constraint(x, pltpu.HBM)
            for x in (
                jnp.transpose(prediction_fields, (1, 2, 0, 3)),
                jnp.transpose(verifying_state, (1, 0, 2)),
                jnp.transpose(normal_state, (1, 0, 2)),
                evaluated_point_flag,
                parallels_each_strip,
            )
        )
    )
    *zonal, a, b, c = pl.pallas_call(
        writer,
        out_shape=[jax.ShapeDtypeStruct((VARS, LEADS, 128), f32)] * 3 + single,
        in_specs=[vmem] * 4,
        out_specs=[hbm] * 6,
        scratch_shapes=[dma((6,))],
        compiler_params=pltpu.CompilerParams(vmem_limit_bytes=2 * 1024 * 1024),
    )(gathered, *means)
    return (*(jnp.transpose(o, (1, 0, 2)) for o in zonal), a, b, c)


def solution(mesh):
    placed = (P(None, None, "lon", "lat"), P(None, "lon", "lat"), P(None, "lon", "lat"), P("lon", "lat"), P())
    return jax.shard_map(
        local,
        mesh=mesh,
        in_specs=placed,
        out_specs=(P(None, None, "lat"), P(None, None, "lat"), P(None, None, "lat"), P(), P(), P()),
        check_vma=False,
    )
```

```python
import math

import jax
import jax.numpy as jnp
from jax import lax
from jax.experimental import pallas as pl
from jax.experimental.pallas import tpu as pltpu
from jax.sharding import PartitionSpec as P

MESH = pl.DeviceIdType.MESH
Y, Z = 4, 8
LEADS, VARS, LONS = 4, 69, 45
GV = 18
PAIRS = 9
PADDED = Y * Z * PAIRS
ROWS = 4 * PAIRS + 3
SCORES = 3 * PAIRS
TILES = 9
OFFS = (4, 3, 5, 2, 6, 1, 7, 0)
NLAT, NLON = 721, 1440
FLOOR = 0.1
SIN_SUM = sum(math.sin(math.pi * g / (NLAT - 1)) for g in range(NLAT))


def kernel(p, t, n, flag, bands, gath, g0, g1, g2,
           pbuf, tnbuf, fbuf, brow, kbuf, wbuf, part, ptru, rel, rel_t, in_m, in_mt, in_p, in_pt, tsum, zout, zin, sbuf,
           lin, hall, lsem, fsem, rel_r, fwd_r, a_r, y_r, sent, got, known):
    lat, j = lax.axis_index("lat"), lax.axis_index("lon")
    nlat = 8
    y, z = j // Z, lax.rem(j, Z)
    up, down, opposite = (lax.rem(y + r, Y) for r in (1, Y - 1, 2))
    f32 = jnp.float32

    def at(yy, zz):
        return yy * Z + zz

    def zto(k):
        return lax.rem(z + OFFS[k], Z)

    def zfrom(k):
        return lax.rem(z + Z - OFFS[k], Z)

    def remote(src, dst, ss, rs, dev):
        return pltpu.make_async_remote_copy(
            src_ref=src, dst_ref=dst, send_sem=ss, recv_sem=rs, device_id=dev, device_id_type=MESH
        )

    def started(ref, sem):
        return pltpu.make_async_copy(ref, ref, sem)

    def load(tile):
        v = pl.ds(jnp.minimum(8 * tile, VARS - 8), 8)
        pltpu.make_async_copy(n.at[:, v], tnbuf.at[tile, 0], lsem.at[0, tile]).start()
        pltpu.make_async_copy(t.at[:, v], tnbuf.at[tile, 1], lsem.at[0, tile]).start()
        pltpu.make_async_copy(p.at[v], pbuf.at[tile], lsem.at[1, tile]).start()

    wrap_up, wrap_down = opposite == 0, opposite == Y - 1
    phases = (
        (2 * opposite, 3),
        (jnp.where(wrap_up, 6, 2 * opposite - 2), jnp.where(wrap_up, 3, 2)),
        (jnp.where(wrap_down, 0, 2 * opposite + 3), jnp.where(wrap_down, 3, 2)),
        (
            jnp.where(wrap_up, 5, jnp.where(opposite == 1, 7, jnp.where(opposite == 2, 0, 3))),
            jnp.where(wrap_up | wrap_down, 1, 2),
        ),
    )

    barrier = pltpu.get_barrier_semaphore()
    Z1, Z2, Y1, Y2, L1, L2 = range(6)
    along_y = [(lat, at(up, z)), (lat, at(down, z))]

    def ring(d):
        return [(lat, at(y, lax.rem(z + d, Z))), (lat, at(y, lax.rem(z + Z - d, Z)))]

    other_core = (lat + 1 - 2 * lax.rem(lat, 2), j)
    bands_near = [other_core, (lax.rem(lat + 2, nlat), j), (lax.rem(lat + nlat - 2, nlat), j)]

    def tell(sem, devices):
        for dev in devices:
            pl.semaphore_signal(sem, inc=1, device_id=dev, device_id_type=MESH)

    tell(barrier, along_y + ring(1) + bands_near)

    def start_loads(phase):
        first, count = phases[phase]

        def go(i, carry):
            load(first + i)
            return carry

        lax.fori_loop(0, count, go, 0)

    small = (pltpu.make_async_copy(flag, fbuf, fsem.at[0]), pltpu.make_async_copy(bands, brow, fsem.at[1]))
    for d in small:
        d.start()
    for phase in range(4):
        start_loads(phase)

    part[:, LEADS * VARS : PADDED] = jnp.zeros((4, PADDED - LEADS * VARS, 128), f32)
    ptru[VARS : Y * GV] = jnp.zeros((Y * GV - VARS, 128), f32)
    for d in small:
        d.wait()
    first, held = jnp.int32(0), jnp.int32(0)
    for b in range(nlat):
        first = first + jnp.where(b < lat, brow[b], 0)
        held = held + jnp.where(b == lat, brow[b], 0)
    lane = lax.broadcasted_iota(jnp.int32, (1, 128), 1)
    for lon in range(LONS):
        kbuf[lon] = jnp.broadcast_to(jnp.where(lane < held, fbuf[lon : lon + 1], 0), (8, 128))
    prows = pbuf.reshape(TILES * 8 * LONS * LEADS, 128)

    def sums(tile):
        top = jnp.minimum(8 * tile, VARS - 8)
        base = tile * (8 * LONS * LEADS)

        def column(lon, totals):
            m = kbuf[lon] != 0
            nn = tnbuf[tile, 0, lon]
            tt = jnp.where(m, tnbuf[tile, 1, lon] - nn, 0.0)
            new = [totals[0] + tt * tt]
            for l in range(LEADS):
                square, offset, product, spread = totals[1 + 4 * l : 5 + 4 * l]
                f = jnp.where(m, prows[pl.ds(base + lon * LEADS + l, 8, stride=LONS * LEADS), :] - nn, 0.0)
                e = f - tt
                new += [square + e * e, offset + e, product + f * tt, spread + f * f]
            return tuple(new)

        def columns(c, totals):
            for u in range(9):
                totals = column(9 * c + u, totals)
            return totals

        totals = lax.fori_loop(0, 5, columns, (jnp.zeros((8, 128), f32),) * 17)
        ptru[pl.ds(top, 8), :] = totals[0]
        for l in range(LEADS):
            for s in range(4):
                part[s, pl.ds(top * LEADS + l, 8, stride=LEADS), :] = totals[1 + 4 * l + s]

    def compute(phase):
        first, count = phases[phase]

        def go(i, carry):
            started(tnbuf.at[first + i], lsem.at[0, first + i]).wait()
            started(pbuf.at[first + i], lsem.at[1, first + i]).wait()
            sums(first + i)
            return carry

        lax.fori_loop(0, count, go, 0)

    def block(g, k):
        return part.at[:, pl.ds(PAIRS * at(g, zto(k)), PAIRS), :]

    def group(g):
        return ptru.at[pl.ds(GV * g, GV), :]

    def take(g, k):
        return part[:, pl.ds(PAIRS * at(g, zto(k)), PAIRS), :]

    REL, DIR, FWD, TRU, ZS, AS, UPS, DOWNS, OPPS, LS, HS = range(11)
    Z_R, DIR_UP, DIR_DOWN, OPP_R, L_R, H_R, TRU_DOWN = range(7)

    def to_relay(k):
        dev = (lat, at(down if k % 2 else up, z))
        if k == Z:
            return remote(group(opposite), rel_t, sent.at[TRU], rel_r.at[k], dev)
        return remote(block(opposite, k), rel.at[k], sent.at[REL], rel_r.at[k], dev)

    def direct(k):
        if k == Z:
            return remote(group(down), in_pt, sent.at[TRU], got.at[TRU_DOWN], (lat, at(down, z)))
        if k % 2:
            return remote(block(up, k), in_m.at[k], sent.at[DIR], got.at[DIR_UP], (lat, at(up, z)))
        return remote(block(down, k), in_p.at[k], sent.at[DIR], got.at[DIR_DOWN], (lat, at(down, z)))

    def relayed(k):
        if k == Z:
            return remote(group(up), in_mt, sent.at[TRU], fwd_r.at[k], (lat, at(up, z)))
        if k % 2:
            return remote(block(down, k), in_p.at[k], sent.at[FWD], fwd_r.at[k], (lat, at(down, z)))
        return remote(block(up, k), in_m.at[k], sent.at[FWD], fwd_r.at[k], (lat, at(up, z)))

    def along_z(k):
        return remote(zout.at[k], zin.at[k], sent.at[ZS], got.at[Z_R], (lat, at(y, zto(k))))

    each = (Z, *range(Z))
    with jax.named_scope("compute_a"):
        compute(0)
    with jax.named_scope("barrier"):
        pl.semaphore_wait(barrier, 7)
    for k in each:
        to_relay(k).start()
    tell(known.at[Z1], ring(1))
    tell(known.at[L1], bands_near)
    with jax.named_scope("compute_b"):
        compute(1)
    for k in range(1, Z, 2):
        direct(k).start()
    with jax.named_scope("known_1"):
        pl.semaphore_wait(known.at[Z1], 2)
        tell(known.at[Z2], ring(2))
        pl.semaphore_wait(known.at[L1], 3)
        tell(known.at[L2], [other_core])
    with jax.named_scope("compute_c"):
        compute(2)
    for k in (Z, *range(0, Z, 2)):
        direct(k).start()
    with jax.named_scope("known_2"):
        pl.semaphore_wait(known.at[Z2], 2)
        tell(known.at[Y1], along_y)
    with jax.named_scope("compute_d"):
        compute(3)
    angle = (first + lane).astype(f32) * (math.pi / (NLAT - 1))
    wbuf[...] = jnp.where(lane < held, jnp.sin(angle) * (NLAT / SIN_SUM), 0.0)
    for k in each:
        with jax.named_scope(f"relay#k={k}"):
            to_relay(k).wait_recv()
            g = down if k % 2 else up
            if k == Z:
                ptru[pl.ds(GV * g, GV), :] = ptru[pl.ds(GV * g, GV), :] + rel_t[...]
            else:
                part[:, pl.ds(PAIRS * at(g, zto(k)), PAIRS), :] = take(g, k) + rel[k]
            relayed(k).start()

    with jax.named_scope("known_3"):
        pl.semaphore_wait(known.at[Y1], 2)
        tell(known.at[Y2], along_y)
        pl.semaphore_wait(known.at[L2], 1)
    direct(Z).wait_recv()
    relayed(Z).wait_recv()
    started(in_m.at[0:4], got.at[DIR_UP]).wait()
    started(in_p.at[0:4], got.at[DIR_DOWN]).wait()
    tsum[...] = ptru[pl.ds(GV * y, GV), :] + (in_mt[...] + in_pt[...])

    def summed(k, out):
        relayed(k).wait_recv()
        x = take(y, k) + (in_m[k] + in_p[k])
        for s in range(4):
            out[PAIRS * s : PAIRS * (s + 1)] = x[s]
        out[4 * PAIRS : ROWS] = tsum[pl.ds((PAIRS * zto(k)) // LEADS, 3), :]

    for k in range(Z - 1):
        with jax.named_scope(f"sum_y#k={k}"):
            summed(k, zout.at[k])
            along_z(k).start()
    summed(Z - 1, sbuf)
    s = sbuf[0:ROWS]
    pl.semaphore_wait(known.at[Y2], 2)
    with jax.named_scope("sum_z"):
        started(zin, got.at[Z_R]).wait()
    for k in range(Z - 1):
        s = s + zin[k]

    c = 1.0 / NLON
    pair = lax.broadcasted_iota(jnp.int32, (PAIRS, 128), 0) + lax.rem(j, 4)
    sbuf[0:ROWS] = s
    square, offset = sbuf[0:9], sbuf[9:18]
    product, spread = sbuf[18:27], sbuf[27:36]
    truth = jnp.where(pair < 4, sbuf[36:37], jnp.where(pair < 8, sbuf[37:38], sbuf[38:39]))
    mine = pl.ds(PAIRS * j, PAIRS)
    gath[0, mine, :] = square * c
    gath[1, mine, :] = offset * c
    gath[2, mine, :] = (product * c) / jnp.sqrt(jnp.maximum(spread * c, FLOOR) * jnp.maximum(truth * c, FLOOR))

    def scores(owner):
        return gath.at[:, pl.ds(PAIRS * owner, PAIRS), :]

    def spread_z(k, owner):
        return remote(scores(owner), scores(owner), sent.at[AS], a_r.at[k], (lat, at(y, zto(k))))

    def to_up(k, owner):
        return remote(scores(owner), scores(owner), sent.at[UPS], y_r.at[k], (lat, at(up, z)))

    def to_down(k, owner):
        return remote(scores(owner), scores(owner), sent.at[DOWNS], y_r.at[k], (lat, at(down, z)))

    def onward(k, owner):
        return remote(scores(owner), scores(owner), sent.at[OPPS], got.at[OPP_R], (lat, at(down if k % 2 else up, z)))

    for k in range(Z - 1):
        spread_z(k, j).start()
    to_up(Z - 1, j).start()
    to_down(Z - 1, j).start()

    sbuf[36:45] = truth
    sbuf[45:48] = jnp.zeros((3, 128), f32)
    column = jnp.sum(sbuf[...] * wbuf[...], axis=1, keepdims=True)
    here = lax.broadcasted_iota(jnp.int32, (48, 128), 0) == lax.broadcasted_iota(jnp.int32, (48, 128), 1)
    lin[lat] = jnp.sum(jnp.where(here, column, 0.0), axis=0, keepdims=True)

    def to_band(d):
        return remote(lin.at[lat], lin.at[lat], sent.at[LS], got.at[L_R], (lax.rem(lat + d, nlat), j))

    def to_all(d):
        return remote(hall.at[j], hall.at[j], sent.at[HS], got.at[H_R], (lat, lax.rem(j + d, Y * Z)))

    for d in range(1, nlat):
        to_band(d).start()
    def from_z(k):
        with jax.named_scope(f"gather_z#k={k}"):
            owner = at(y, zfrom(k))
            spread_z(k, owner).wait_recv()
            to_up(k, owner).start()
            to_down(k, owner).start()

    def from_y(k):
        with jax.named_scope(f"gather_y#k={k}"):
            below, above = at(down, zfrom(k)), at(up, zfrom(k))
            started(gath.at[0, 0 : 2 * SCORES], y_r.at[k]).wait()
            onward(k, above if k % 2 else below).start()

    near = (5, 6, 3, 4, 1, 2, 0)
    for k in near[:2]:
        from_z(k)
    from_y(Z - 1)
    for k in near[2:]:
        from_z(k)
    with jax.named_scope("bands"):
        started(lin.at[0 : nlat - 1], got.at[L_R]).wait()
    total = lin[0]
    for b in range(1, nlat):
        total = total + lin[b]
    total = total * (1.0 / (NLAT * NLON))
    over = pltpu.roll(total, 128 - 9, 1)
    under = pltpu.roll(total, 128 - 18, 1)
    skill = total / jnp.sqrt(jnp.maximum(over, FLOOR) * jnp.maximum(under, FLOOR))
    measures = jnp.where(lane < 9, jnp.sqrt(jnp.maximum(total, FLOOR)), jnp.where(lane < 18, total, skill))
    hall[j] = jnp.where(lane < SCORES, measures, 0.0)
    for d in range(1, Y * Z):
        to_all(d).start()

    for k in near:
        from_y(k)
    with jax.named_scope("globals"):
        started(hall.at[0 : Y * Z - 1], got.at[H_R]).wait()
    table = hall[:, 0, :]
    owner = lax.broadcasted_iota(jnp.int32, (Y * Z, 128), 0)
    var = lax.broadcasted_iota(jnp.int32, (Y * Z, 128), 1)
    chosen = []
    for l in range(LEADS):
        mine = lax.shift_right_logical((var * LEADS + l) * 7282, 16)
        chosen.append(jnp.where(mine == owner, 1.0, 0.0))
    every = lax.dot_general(
        table,
        jnp.concatenate(chosen, axis=1),
        (((0,), (0,)), ((), ())),
        precision=lax.Precision.HIGHEST,
        preferred_element_type=f32,
    )
    for l in range(LEADS):
        q = var * LEADS + l
        picked = every[0 : Y * Z, 128 * l : 128 * (l + 1)]
        rest = q - lax.shift_right_logical(q * 7282, 16) * PAIRS
        for m, g in enumerate((g0, g1, g2)):
            line = jnp.sum(jnp.where(owner == rest + m * PAIRS, picked, 0.0), axis=0, keepdims=True)
            g[l : l + 1, :] = line[:, 0:VARS]

    with jax.named_scope("gather_o"):
        started(gath.at[0, 0 : Z * SCORES], got.at[OPP_R]).wait()

    with jax.named_scope("sends"):
        for i, ref in (
            (REL, rel),
            (DIR, rel),
            (FWD, rel),
            (TRU, ptru.at[0 : 3 * GV]),
            (ZS, zin),
            (AS, gath.at[0, 0 : (Z - 1) * SCORES]),
            (UPS, gath.at[0, 0 : Z * SCORES]),
            (DOWNS, gath.at[0, 0 : Z * SCORES]),
            (OPPS, gath.at[0, 0 : Z * SCORES]),
            (LS, hall.at[0 : nlat - 1]),
            (HS, hall.at[0 : Y * Z - 1]),
        ):
            started(ref, sent.at[i]).wait()


def writer(gath, s0, s1, s2, o0, o1, o2, g0, g1, g2, sems):
    rows = LEADS * VARS
    copies = [
        pltpu.make_async_copy(gath.at[m, pl.ds(0, rows)], o.reshape(rows, 128), sems.at[m])
        for m, o in enumerate((o0, o1, o2))
    ]
    copies += [
        pltpu.make_async_copy(s, g, sems.at[3 + m]) for m, (s, g) in enumerate(((s0, g0), (s1, g1), (s2, g2)))
    ]
    for c in copies:
        c.start()
    for c in copies:
        c.wait()


def local(prediction_fields, verifying_state, normal_state, evaluated_point_flag, parallels_each_strip):
    f32 = jnp.float32
    hbm, vmem = pl.BlockSpec(memory_space=pltpu.HBM), pl.BlockSpec(memory_space=pltpu.VMEM)
    dma = pltpu.SemaphoreType.DMA
    single = [jax.ShapeDtypeStruct((LEADS, VARS), f32)] * 3
    gathered, *means = pl.pallas_call(
        kernel,
        out_shape=[jax.ShapeDtypeStruct((3, PADDED, 128), f32)] + single,
        in_specs=[hbm] * 5,
        out_specs=[vmem] * 4,
        scratch_shapes=[
            pltpu.VMEM((TILES, 8, LONS, LEADS, 128), f32),
            pltpu.VMEM((TILES, 2, LONS, 8, 128), f32),
            pltpu.VMEM((LONS, 128), jnp.int32),
            pltpu.SMEM((8,), jnp.int32),
            pltpu.VMEM((LONS, 8, 128), jnp.int32),
            pltpu.VMEM((1, 128), f32),
            pltpu.VMEM((4, PADDED, 128), f32),
            pltpu.VMEM((Y * GV, 128), f32),
            *[pltpu.VMEM((Z, 4, PAIRS, 128), f32), pltpu.VMEM((GV, 128), f32)] * 3,
            pltpu.VMEM((GV, 128), f32),
            pltpu.VMEM((Z - 1, ROWS, 128), f32),
            pltpu.VMEM((Z - 1, ROWS, 128), f32),
            pltpu.VMEM((48, 128), f32),
            pltpu.VMEM((8, 1, 128), f32),
            pltpu.VMEM((Y * Z, 1, 128), f32),
            dma((2, TILES)),
            dma((2,)),
            *[dma((Z + 1,))] * 2,
            dma((Z - 1,)),
            dma((Z,)),
            dma((11,)),
            dma((7,)),
            pltpu.SemaphoreType.REGULAR((6,)),
        ],
        compiler_params=pltpu.CompilerParams(
            collective_id=0, has_side_effects=True, vmem_limit_bytes=32 * 1024 * 1024
        ),
    )(
        *(
            pltpu.with_memory_space_constraint(x, pltpu.HBM)
            for x in (
                jnp.transpose(prediction_fields, (1, 2, 0, 3)),
                jnp.transpose(verifying_state, (1, 0, 2)),
                jnp.transpose(normal_state, (1, 0, 2)),
                evaluated_point_flag,
                parallels_each_strip,
            )
        )
    )
    *zonal, a, b, c = pl.pallas_call(
        writer,
        out_shape=[jax.ShapeDtypeStruct((VARS, LEADS, 128), f32)] * 3 + single,
        in_specs=[vmem] * 4,
        out_specs=[hbm] * 6,
        scratch_shapes=[dma((6,))],
        compiler_params=pltpu.CompilerParams(vmem_limit_bytes=2 * 1024 * 1024),
    )(gathered, *means)
    return (*(jnp.transpose(o, (1, 0, 2)) for o in zonal), a, b, c)


def solution(mesh):
    placed = (P(None, None, "lon", "lat"), P(None, "lon", "lat"), P(None, "lon", "lat"), P("lon", "lat"), P())
    return jax.shard_map(
        local,
        mesh=mesh,
        in_specs=placed,
        out_specs=(P(None, None, "lat"), P(None, None, "lat"), P(None, None, "lat"), P(), P(), P()),
        check_vma=False,
    )
```

```python
import math

import jax
import jax.numpy as jnp
from jax import lax
from jax.experimental import pallas as pl
from jax.experimental.pallas import tpu as pltpu
from jax.sharding import PartitionSpec as P

MESH = pl.DeviceIdType.MESH
Y, Z = 4, 8
LEADS, VARS, LONS = 4, 69, 45
GV = 18
PAIRS = 9
PADDED = Y * Z * PAIRS
ROWS = 4 * PAIRS + 3
SCORES = 3 * PAIRS
TILES = 9
OFFS = (4, 3, 5, 2, 6, 1, 7, 0)
NLAT, NLON = 721, 1440
FLOOR = 0.1
SIN_SUM = sum(math.sin(math.pi * g / (NLAT - 1)) for g in range(NLAT))


def kernel(p, t, n, flag, bands, gath, g0, g1, g2,
           pbuf, tnbuf, fbuf, brow, kbuf, wbuf, part, ptru, rel, rel_t, in_m, in_mt, in_p, in_pt, tsum, zout, zin, sbuf,
           lin, hall, lsem, fsem, rel_r, fwd_r, a_r, y_r, sent, got, known):
    lat, j = lax.axis_index("lat"), lax.axis_index("lon")
    nlat = 8
    y, z = j // Z, lax.rem(j, Z)
    up, down, opposite = (lax.rem(y + r, Y) for r in (1, Y - 1, 2))
    f32 = jnp.float32

    def at(yy, zz):
        return yy * Z + zz

    def zto(k):
        return lax.rem(z + OFFS[k], Z)

    def zfrom(k):
        return lax.rem(z + Z - OFFS[k], Z)

    def remote(src, dst, ss, rs, dev):
        return pltpu.make_async_remote_copy(
            src_ref=src, dst_ref=dst, send_sem=ss, recv_sem=rs, device_id=dev, device_id_type=MESH
        )

    def started(ref, sem):
        return pltpu.make_async_copy(ref, ref, sem)

    def load(tile):
        v = pl.ds(jnp.minimum(8 * tile, VARS - 8), 8)
        pltpu.make_async_copy(n.at[:, v], tnbuf.at[tile, 0], lsem.at[0, tile]).start()
        pltpu.make_async_copy(t.at[:, v], tnbuf.at[tile, 1], lsem.at[0, tile]).start()
        pltpu.make_async_copy(p.at[v], pbuf.at[tile], lsem.at[1, tile]).start()

    wrap_up, wrap_down = opposite == 0, opposite == Y - 1
    phases = (
        (2 * opposite, 3),
        (jnp.where(wrap_up, 6, 2 * opposite - 2), jnp.where(wrap_up, 3, 2)),
        (jnp.where(wrap_down, 0, 2 * opposite + 3), jnp.where(wrap_down, 3, 2)),
        (
            jnp.where(wrap_up, 5, jnp.where(opposite == 1, 7, jnp.where(opposite == 2, 0, 3))),
            jnp.where(wrap_up | wrap_down, 1, 2),
        ),
    )

    barrier = pltpu.get_barrier_semaphore()
    Z1, Z2, Y1, Y2, L1, L2 = range(6)
    along_y = [(lat, at(up, z)), (lat, at(down, z))]

    def ring(d):
        return [(lat, at(y, lax.rem(z + d, Z))), (lat, at(y, lax.rem(z + Z - d, Z)))]

    other_core = (lat + 1 - 2 * lax.rem(lat, 2), j)
    bands_near = [other_core, (lax.rem(lat + 2, nlat), j), (lax.rem(lat + nlat - 2, nlat), j)]

    def tell(sem, devices):
        for dev in devices:
            pl.semaphore_signal(sem, inc=1, device_id=dev, device_id_type=MESH)

    tell(barrier, along_y + ring(1) + bands_near)

    def start_loads(phase):
        first, count = phases[phase]

        def go(i, carry):
            load(first + i)
            return carry

        lax.fori_loop(0, count, go, 0)

    small = (pltpu.make_async_copy(flag, fbuf, fsem.at[0]), pltpu.make_async_copy(bands, brow, fsem.at[1]))
    for d in small:
        d.start()
    for phase in range(4):
        start_loads(phase)

    part[:, LEADS * VARS : PADDED] = jnp.zeros((4, PADDED - LEADS * VARS, 128), f32)
    ptru[VARS : Y * GV] = jnp.zeros((Y * GV - VARS, 128), f32)
    for d in small:
        d.wait()
    first, held = jnp.int32(0), jnp.int32(0)
    for b in range(nlat):
        first = first + jnp.where(b < lat, brow[b], 0)
        held = held + jnp.where(b == lat, brow[b], 0)
    lane = lax.broadcasted_iota(jnp.int32, (1, 128), 1)
    for lon in range(LONS):
        kbuf[lon] = jnp.broadcast_to(jnp.where(lane < held, fbuf[lon : lon + 1], 0), (8, 128))
    prows = pbuf.reshape(TILES * 8 * LONS * LEADS, 128)

    def sums(tile):
        top = jnp.minimum(8 * tile, VARS - 8)
        base = tile * (8 * LONS * LEADS)

        def column(lon, totals):
            m = kbuf[lon] != 0
            nn = tnbuf[tile, 0, lon]
            tt = jnp.where(m, tnbuf[tile, 1, lon] - nn, 0.0)
            new = [totals[0] + tt * tt]
            for l in range(LEADS):
                square, offset, product, spread = totals[1 + 4 * l : 5 + 4 * l]
                f = jnp.where(m, prows[pl.ds(base + lon * LEADS + l, 8, stride=LONS * LEADS), :] - nn, 0.0)
                e = f - tt
                new += [square + e * e, offset + e, product + f * tt, spread + f * f]
            return tuple(new)

        def columns(c, totals):
            for u in range(9):
                totals = column(9 * c + u, totals)
            return totals

        totals = lax.fori_loop(0, 5, columns, (jnp.zeros((8, 128), f32),) * 17)
        ptru[pl.ds(top, 8), :] = totals[0]
        for l in range(LEADS):
            for s in range(4):
                part[s, pl.ds(top * LEADS + l, 8, stride=LEADS), :] = totals[1 + 4 * l + s]

    def compute(phase):
        first, count = phases[phase]

        def go(i, carry):
            started(tnbuf.at[first + i], lsem.at[0, first + i]).wait()
            started(pbuf.at[first + i], lsem.at[1, first + i]).wait()
            sums(first + i)
            return carry

        lax.fori_loop(0, count, go, 0)

    def block(g, k):
        return part.at[:, pl.ds(PAIRS * at(g, zto(k)), PAIRS), :]

    def group(g):
        return ptru.at[pl.ds(GV * g, GV), :]

    def take(g, k):
        return part[:, pl.ds(PAIRS * at(g, zto(k)), PAIRS), :]

    REL, DIR, FWD, TRU, ZS, AS, UPS, DOWNS, OPPS, LS, HS = range(11)
    Z_R, DIR_UP, DIR_DOWN, OPP_R, L_R, H_R, TRU_DOWN = range(7)

    def to_relay(k):
        dev = (lat, at(down if k % 2 else up, z))
        if k == Z:
            return remote(group(opposite), rel_t, sent.at[TRU], rel_r.at[k], dev)
        return remote(block(opposite, k), rel.at[k], sent.at[REL], rel_r.at[k], dev)

    def direct(k):
        if k == Z:
            return remote(group(down), in_pt, sent.at[TRU], got.at[TRU_DOWN], (lat, at(down, z)))
        if k % 2:
            return remote(block(up, k), in_m.at[k], sent.at[DIR], got.at[DIR_UP], (lat, at(up, z)))
        return remote(block(down, k), in_p.at[k], sent.at[DIR], got.at[DIR_DOWN], (lat, at(down, z)))

    def relayed(k):
        if k == Z:
            return remote(group(up), in_mt, sent.at[TRU], fwd_r.at[k], (lat, at(up, z)))
        if k % 2:
            return remote(block(down, k), in_p.at[k], sent.at[FWD], fwd_r.at[k], (lat, at(down, z)))
        return remote(block(up, k), in_m.at[k], sent.at[FWD], fwd_r.at[k], (lat, at(up, z)))

    def along_z(k):
        return remote(zout.at[k], zin.at[k], sent.at[ZS], got.at[Z_R], (lat, at(y, zto(k))))

    each = (Z, *range(Z))
    with jax.named_scope("compute_a"):
        compute(0)
    with jax.named_scope("barrier"):
        pl.semaphore_wait(barrier, 7)
    for k in each:
        to_relay(k).start()
    tell(known.at[Z1], ring(1))
    tell(known.at[L1], bands_near)
    with jax.named_scope("compute_b"):
        compute(1)
    for k in range(1, Z, 2):
        direct(k).start()
    with jax.named_scope("compute_c"):
        compute(2)
    for k in (Z, *range(0, Z, 2)):
        direct(k).start()
    with jax.named_scope("compute_d"):
        compute(3)
    angle = (first + lane).astype(f32) * (math.pi / (NLAT - 1))
    wbuf[...] = jnp.where(lane < held, jnp.sin(angle) * (NLAT / SIN_SUM), 0.0)
    with jax.named_scope("known_1"):
        pl.semaphore_wait(known.at[Z1], 2)
        tell(known.at[Z2], ring(2))
    for k in each:
        with jax.named_scope(f"relay#k={k}"):
            to_relay(k).wait_recv()
            g = down if k % 2 else up
            if k == Z:
                ptru[pl.ds(GV * g, GV), :] = ptru[pl.ds(GV * g, GV), :] + rel_t[...]
            else:
                part[:, pl.ds(PAIRS * at(g, zto(k)), PAIRS), :] = take(g, k) + rel[k]
            relayed(k).start()

    with jax.named_scope("known_2"):
        pl.semaphore_wait(known.at[Z2], 2)
        tell(known.at[Y1], along_y)
    direct(Z).wait_recv()
    relayed(Z).wait_recv()
    started(in_m.at[0:4], got.at[DIR_UP]).wait()
    started(in_p.at[0:4], got.at[DIR_DOWN]).wait()
    tsum[...] = ptru[pl.ds(GV * y, GV), :] + (in_mt[...] + in_pt[...])

    def summed(k, out):
        relayed(k).wait_recv()
        x = take(y, k) + (in_m[k] + in_p[k])
        for s in range(4):
            out[PAIRS * s : PAIRS * (s + 1)] = x[s]
        out[4 * PAIRS : ROWS] = tsum[pl.ds((PAIRS * zto(k)) // LEADS, 3), :]

    for k in range(Z - 1):
        with jax.named_scope(f"sum_y#k={k}"):
            summed(k, zout.at[k])
            along_z(k).start()
    summed(Z - 1, sbuf)
    s = sbuf[0:ROWS]
    with jax.named_scope("known_3"):
        pl.semaphore_wait(known.at[L1], 3)
        tell(known.at[L2], [other_core])
        pl.semaphore_wait(known.at[Y1], 2)
        tell(known.at[Y2], along_y)
    with jax.named_scope("sum_z"):
        started(zin, got.at[Z_R]).wait()
    for k in range(Z - 1):
        s = s + zin[k]

    c = 1.0 / NLON
    pair = lax.broadcasted_iota(jnp.int32, (PAIRS, 128), 0) + lax.rem(j, 4)
    sbuf[0:ROWS] = s
    square, offset = sbuf[0:9], sbuf[9:18]
    product, spread = sbuf[18:27], sbuf[27:36]
    truth = jnp.where(pair < 4, sbuf[36:37], jnp.where(pair < 8, sbuf[37:38], sbuf[38:39]))
    mine = pl.ds(PAIRS * j, PAIRS)
    gath[0, mine, :] = square * c
    gath[1, mine, :] = offset * c
    gath[2, mine, :] = (product * c) / jnp.sqrt(jnp.maximum(spread * c, FLOOR) * jnp.maximum(truth * c, FLOOR))

    def scores(owner):
        return gath.at[:, pl.ds(PAIRS * owner, PAIRS), :]

    def spread_z(k, owner):
        return remote(scores(owner), scores(owner), sent.at[AS], a_r.at[k], (lat, at(y, zto(k))))

    def to_up(k, owner):
        return remote(scores(owner), scores(owner), sent.at[UPS], y_r.at[k], (lat, at(up, z)))

    def to_down(k, owner):
        return remote(scores(owner), scores(owner), sent.at[DOWNS], y_r.at[k], (lat, at(down, z)))

    def onward(k, owner):
        return remote(scores(owner), scores(owner), sent.at[OPPS], got.at[OPP_R], (lat, at(down if k % 2 else up, z)))

    for k in range(Z - 1):
        spread_z(k, j).start()
    to_up(Z - 1, j).start()
    to_down(Z - 1, j).start()

    sbuf[36:45] = truth
    sbuf[45:48] = jnp.zeros((3, 128), f32)
    column = jnp.sum(sbuf[...] * wbuf[...], axis=1, keepdims=True)
    here = lax.broadcasted_iota(jnp.int32, (48, 128), 0) == lax.broadcasted_iota(jnp.int32, (48, 128), 1)
    lin[lat] = jnp.sum(jnp.where(here, column, 0.0), axis=0, keepdims=True)

    def to_band(d):
        return remote(lin.at[lat], lin.at[lat], sent.at[LS], got.at[L_R], (lax.rem(lat + d, nlat), j))

    def to_all(d):
        return remote(hall.at[j], hall.at[j], sent.at[HS], got.at[H_R], (lat, lax.rem(j + d, Y * Z)))

    pl.semaphore_wait(known.at[L2], 1)
    for d in range(1, nlat):
        to_band(d).start()
    def from_z(k):
        with jax.named_scope(f"gather_z#k={k}"):
            owner = at(y, zfrom(k))
            spread_z(k, owner).wait_recv()
            to_up(k, owner).start()
            to_down(k, owner).start()

    def from_y(k):
        with jax.named_scope(f"gather_y#k={k}"):
            below, above = at(down, zfrom(k)), at(up, zfrom(k))
            started(gath.at[0, 0 : 2 * SCORES], y_r.at[k]).wait()
            onward(k, above if k % 2 else below).start()

    near = (5, 6, 3, 4, 1, 2, 0)
    for k in near[:2]:
        from_z(k)
    from_y(Z - 1)
    for k in near[2:]:
        from_z(k)
    with jax.named_scope("bands"):
        started(lin.at[0 : nlat - 1], got.at[L_R]).wait()
    total = lin[0]
    for b in range(1, nlat):
        total = total + lin[b]
    total = total * (1.0 / (NLAT * NLON))
    over = pltpu.roll(total, 128 - 9, 1)
    under = pltpu.roll(total, 128 - 18, 1)
    skill = total / jnp.sqrt(jnp.maximum(over, FLOOR) * jnp.maximum(under, FLOOR))
    measures = jnp.where(lane < 9, jnp.sqrt(jnp.maximum(total, FLOOR)), jnp.where(lane < 18, total, skill))
    hall[j] = jnp.where(lane < SCORES, measures, 0.0)
    pl.semaphore_wait(known.at[Y2], 2)
    for d in range(1, Y * Z):
        to_all(d).start()

    for k in near:
        from_y(k)
    with jax.named_scope("globals"):
        started(hall.at[0 : Y * Z - 1], got.at[H_R]).wait()
    table = hall[:, 0, :]
    owner = lax.broadcasted_iota(jnp.int32, (Y * Z, 128), 0)
    var = lax.broadcasted_iota(jnp.int32, (Y * Z, 128), 1)
    chosen = []
    for l in range(LEADS):
        mine = lax.shift_right_logical((var * LEADS + l) * 7282, 16)
        chosen.append(jnp.where(mine == owner, 1.0, 0.0))
    every = lax.dot_general(
        table,
        jnp.concatenate(chosen, axis=1),
        (((0,), (0,)), ((), ())),
        precision=lax.Precision.HIGHEST,
        preferred_element_type=f32,
    )
    for l in range(LEADS):
        q = var * LEADS + l
        picked = every[0 : Y * Z, 128 * l : 128 * (l + 1)]
        rest = q - lax.shift_right_logical(q * 7282, 16) * PAIRS
        for m, g in enumerate((g0, g1, g2)):
            line = jnp.sum(jnp.where(owner == rest + m * PAIRS, picked, 0.0), axis=0, keepdims=True)
            g[l : l + 1, :] = line[:, 0:VARS]

    with jax.named_scope("gather_o"):
        started(gath.at[0, 0 : Z * SCORES], got.at[OPP_R]).wait()

    with jax.named_scope("sends"):
        for i, ref in (
            (REL, rel),
            (DIR, rel),
            (FWD, rel),
            (TRU, ptru.at[0 : 3 * GV]),
            (ZS, zin),
            (AS, gath.at[0, 0 : (Z - 1) * SCORES]),
            (UPS, gath.at[0, 0 : Z * SCORES]),
            (DOWNS, gath.at[0, 0 : Z * SCORES]),
            (OPPS, gath.at[0, 0 : Z * SCORES]),
            (LS, hall.at[0 : nlat - 1]),
            (HS, hall.at[0 : Y * Z - 1]),
        ):
            started(ref, sent.at[i]).wait()


def writer(gath, s0, s1, s2, o0, o1, o2, g0, g1, g2, sems):
    rows = LEADS * VARS
    copies = [
        pltpu.make_async_copy(gath.at[m, pl.ds(0, rows)], o.reshape(rows, 128), sems.at[m])
        for m, o in enumerate((o0, o1, o2))
    ]
    copies += [
        pltpu.make_async_copy(s, g, sems.at[3 + m]) for m, (s, g) in enumerate(((s0, g0), (s1, g1), (s2, g2)))
    ]
    for c in copies:
        c.start()
    for c in copies:
        c.wait()


def local(prediction_fields, verifying_state, normal_state, evaluated_point_flag, parallels_each_strip):
    f32 = jnp.float32
    hbm, vmem = pl.BlockSpec(memory_space=pltpu.HBM), pl.BlockSpec(memory_space=pltpu.VMEM)
    dma = pltpu.SemaphoreType.DMA
    single = [jax.ShapeDtypeStruct((LEADS, VARS), f32)] * 3
    gathered, *means = pl.pallas_call(
        kernel,
        out_shape=[jax.ShapeDtypeStruct((3, PADDED, 128), f32)] + single,
        in_specs=[hbm] * 5,
        out_specs=[vmem] * 4,
        scratch_shapes=[
            pltpu.VMEM((TILES, 8, LONS, LEADS, 128), f32),
            pltpu.VMEM((TILES, 2, LONS, 8, 128), f32),
            pltpu.VMEM((LONS, 128), jnp.int32),
            pltpu.SMEM((8,), jnp.int32),
            pltpu.VMEM((LONS, 8, 128), jnp.int32),
            pltpu.VMEM((1, 128), f32),
            pltpu.VMEM((4, PADDED, 128), f32),
            pltpu.VMEM((Y * GV, 128), f32),
            *[pltpu.VMEM((Z, 4, PAIRS, 128), f32), pltpu.VMEM((GV, 128), f32)] * 3,
            pltpu.VMEM((GV, 128), f32),
            pltpu.VMEM((Z - 1, ROWS, 128), f32),
            pltpu.VMEM((Z - 1, ROWS, 128), f32),
            pltpu.VMEM((48, 128), f32),
            pltpu.VMEM((8, 1, 128), f32),
            pltpu.VMEM((Y * Z, 1, 128), f32),
            dma((2, TILES)),
            dma((2,)),
            *[dma((Z + 1,))] * 2,
            dma((Z - 1,)),
            dma((Z,)),
            dma((11,)),
            dma((7,)),
            pltpu.SemaphoreType.REGULAR((6,)),
        ],
        compiler_params=pltpu.CompilerParams(
            collective_id=0, has_side_effects=True, vmem_limit_bytes=32 * 1024 * 1024
        ),
    )(
        *(
            pltpu.with_memory_space_constraint(x, pltpu.HBM)
            for x in (
                jnp.transpose(prediction_fields, (1, 2, 0, 3)),
                jnp.transpose(verifying_state, (1, 0, 2)),
                jnp.transpose(normal_state, (1, 0, 2)),
                evaluated_point_flag,
                parallels_each_strip,
            )
        )
    )
    *zonal, a, b, c = pl.pallas_call(
        writer,
        out_shape=[jax.ShapeDtypeStruct((VARS, LEADS, 128), f32)] * 3 + single,
        in_specs=[vmem] * 4,
        out_specs=[hbm] * 6,
        scratch_shapes=[dma((6,))],
        compiler_params=pltpu.CompilerParams(vmem_limit_bytes=2 * 1024 * 1024),
    )(gathered, *means)
    return (*(jnp.transpose(o, (1, 0, 2)) for o in zonal), a, b, c)


def solution(mesh):
    placed = (P(None, None, "lon", "lat"), P(None, "lon", "lat"), P(None, "lon", "lat"), P("lon", "lat"), P())
    return jax.shard_map(
        local,
        mesh=mesh,
        in_specs=placed,
        out_specs=(P(None, None, "lat"), P(None, None, "lat"), P(None, None, "lat"), P(), P(), P()),
        check_vma=False,
    )
```

```python
import math

import jax
import jax.numpy as jnp
from jax import lax
from jax.experimental import pallas as pl
from jax.experimental.pallas import tpu as pltpu
from jax.sharding import PartitionSpec as P

MESH = pl.DeviceIdType.MESH
Y, Z = 4, 8
LEADS, VARS, LONS = 4, 69, 45
GV = 18
PAIRS = 9
PADDED = Y * Z * PAIRS
ROWS = 4 * PAIRS + 3
SCORES = 3 * PAIRS
TILES = 9
OFFS = (4, 3, 5, 2, 6, 1, 7, 0)
NLAT, NLON = 721, 1440
FLOOR = 0.1
SIN_SUM = sum(math.sin(math.pi * g / (NLAT - 1)) for g in range(NLAT))


def kernel(p, t, n, flag, bands, gath, g0, g1, g2,
           pbuf, tnbuf, fbuf, brow, kbuf, wbuf, part, ptru, rel, rel_t, in_m, in_mt, in_p, in_pt, tsum, zout, zin, sbuf,
           lin, hall, lsem, fsem, rel_r, fwd_r, a_r, sent, got, known):
    lat, j = lax.axis_index("lat"), lax.axis_index("lon")
    nlat = 8
    y, z = j // Z, lax.rem(j, Z)
    up, down, opposite = (lax.rem(y + r, Y) for r in (1, Y - 1, 2))
    f32 = jnp.float32

    def at(yy, zz):
        return yy * Z + zz

    def zto(k):
        return lax.rem(z + OFFS[k], Z)

    def zfrom(k):
        return lax.rem(z + Z - OFFS[k], Z)

    def remote(src, dst, ss, rs, dev):
        return pltpu.make_async_remote_copy(
            src_ref=src, dst_ref=dst, send_sem=ss, recv_sem=rs, device_id=dev, device_id_type=MESH
        )

    def started(ref, sem):
        return pltpu.make_async_copy(ref, ref, sem)

    def load(tile):
        v = pl.ds(jnp.minimum(8 * tile, VARS - 8), 8)
        pltpu.make_async_copy(n.at[:, v], tnbuf.at[tile, 0], lsem.at[tile]).start()
        pltpu.make_async_copy(t.at[:, v], tnbuf.at[tile, 1], lsem.at[tile]).start()
        pltpu.make_async_copy(p.at[v], pbuf.at[tile], lsem.at[tile]).start()

    wrap_up, wrap_down = opposite == 0, opposite == Y - 1
    phases = (
        (2 * opposite, 3),
        (jnp.where(wrap_up, 6, 2 * opposite - 2), jnp.where(wrap_up, 3, 2)),
        (jnp.where(wrap_down, 0, 2 * opposite + 3), jnp.where(wrap_down, 3, 2)),
        (
            jnp.where(wrap_up, 5, jnp.where(opposite == 1, 7, jnp.where(opposite == 2, 0, 3))),
            jnp.where(wrap_up | wrap_down, 1, 2),
        ),
    )

    barrier = pltpu.get_barrier_semaphore()
    Z1, Z2, Y1, Y2, L1, L2 = range(6)
    beside = [(lat, at(up, z)), (lat, at(down, z))]

    def ring(d):
        return [(lat, at(y, lax.rem(z + d, Z))), (lat, at(y, lax.rem(z + Z - d, Z)))]

    other_core = (lat + 1 - 2 * lax.rem(lat, 2), j)
    bands_near = [other_core, (lax.rem(lat + 2, nlat), j), (lax.rem(lat + nlat - 2, nlat), j)]

    def tell(sem, devices):
        for dev in devices:
            pl.semaphore_signal(sem, inc=1, device_id=dev, device_id_type=MESH)

    tell(barrier, beside + ring(1) + bands_near)

    def start_loads(phase):
        first, count = phases[phase]

        def go(i, carry):
            load(first + i)
            return carry

        lax.fori_loop(0, count, go, 0)

    small = (pltpu.make_async_copy(flag, fbuf, fsem.at[0]), pltpu.make_async_copy(bands, brow, fsem.at[1]))
    for d in small:
        d.start()
    for phase in range(4):
        start_loads(phase)

    part[:, LEADS * VARS : PADDED] = jnp.zeros((4, PADDED - LEADS * VARS, 128), f32)
    ptru[VARS : Y * GV] = jnp.zeros((Y * GV - VARS, 128), f32)
    for d in small:
        d.wait()
    first, held = jnp.int32(0), jnp.int32(0)
    for b in range(nlat):
        first = first + jnp.where(b < lat, brow[b], 0)
        held = held + jnp.where(b == lat, brow[b], 0)
    lane = lax.broadcasted_iota(jnp.int32, (1, 128), 1)
    for lon in range(LONS):
        kbuf[lon] = jnp.broadcast_to(jnp.where(lane < held, fbuf[lon : lon + 1], 0), (8, 128))
    prows = pbuf.reshape(TILES * 8 * LONS * LEADS, 128)

    def sums(tile):
        top = jnp.minimum(8 * tile, VARS - 8)
        base = tile * (8 * LONS * LEADS)

        def column(lon, totals):
            m = kbuf[lon] != 0
            nn = tnbuf[tile, 0, lon]
            tt = jnp.where(m, tnbuf[tile, 1, lon] - nn, 0.0)
            new = [totals[0] + tt * tt]
            for l in range(LEADS):
                square, offset, product, spread = totals[1 + 4 * l : 5 + 4 * l]
                f = jnp.where(m, prows[pl.ds(base + lon * LEADS + l, 8, stride=LONS * LEADS), :] - nn, 0.0)
                e = f - tt
                new += [square + e * e, offset + e, product + f * tt, spread + f * f]
            return tuple(new)

        def columns(c, totals):
            for u in range(9):
                totals = column(9 * c + u, totals)
            return totals

        totals = lax.fori_loop(0, 5, columns, (jnp.zeros((8, 128), f32),) * 17)
        ptru[pl.ds(top, 8), :] = totals[0]
        for l in range(LEADS):
            for s in range(4):
                part[s, pl.ds(top * LEADS + l, 8, stride=LEADS), :] = totals[1 + 4 * l + s]

    def compute(phase):
        first, count = phases[phase]

        def go(i, carry):
            started(prows.at[pl.ds(0, 8 * LONS * (LEADS + 2))], lsem.at[first + i]).wait()
            sums(first + i)
            return carry

        lax.fori_loop(0, count, go, 0)

    def block(g, k):
        return part.at[:, pl.ds(PAIRS * at(g, zto(k)), PAIRS), :]

    def group(g):
        return ptru.at[pl.ds(GV * g, GV), :]

    def take(g, k):
        return part[:, pl.ds(PAIRS * at(g, zto(k)), PAIRS), :]

    Z_R, DIR_UP, DIR_DOWN, OPP_R, L_R, H_R, TRU_DOWN, Y_R = range(8)

    def to_relay(k):
        dev = (lat, at(down if k % 2 else up, z))
        if k == Z:
            return remote(group(opposite), rel_t, sent.at[0], rel_r.at[k], dev)
        return remote(block(opposite, k), rel.at[k], sent.at[0], rel_r.at[k], dev)

    def direct(k):
        if k == Z:
            return remote(group(down), in_pt, sent.at[0], got.at[TRU_DOWN], (lat, at(down, z)))
        if k % 2:
            return remote(block(up, k), in_m.at[k], sent.at[0], got.at[DIR_UP], (lat, at(up, z)))
        return remote(block(down, k), in_p.at[k], sent.at[0], got.at[DIR_DOWN], (lat, at(down, z)))

    def relayed(k):
        if k == Z:
            return remote(group(up), in_mt, sent.at[0], fwd_r.at[k], (lat, at(up, z)))
        if k % 2:
            return remote(block(down, k), in_p.at[k], sent.at[0], fwd_r.at[k], (lat, at(down, z)))
        return remote(block(up, k), in_m.at[k], sent.at[0], fwd_r.at[k], (lat, at(up, z)))

    def along_z(k):
        return remote(zout.at[k], zin.at[k], sent.at[0], got.at[Z_R], (lat, at(y, zto(k))))

    each = (Z, *range(Z))
    with jax.named_scope("compute_a"):
        compute(0)
    with jax.named_scope("barrier"):
        pl.semaphore_wait(barrier, 7)
    for k in each:
        to_relay(k).start()
    tell(known.at[Z1], ring(1))
    tell(known.at[L1], bands_near)
    with jax.named_scope("compute_b"):
        compute(1)
    for k in range(1, Z, 2):
        direct(k).start()
    with jax.named_scope("compute_c"):
        compute(2)
    for k in (Z, *range(0, Z, 2)):
        direct(k).start()
    with jax.named_scope("compute_d"):
        compute(3)
    angle = (first + lane).astype(f32) * (math.pi / (NLAT - 1))
    wbuf[...] = jnp.where(lane < held, jnp.sin(angle) * (NLAT / SIN_SUM), 0.0)
    with jax.named_scope("known_1"):
        pl.semaphore_wait(known.at[Z1], 2)
        tell(known.at[Z2], ring(2))
    def relay(k):
        with jax.named_scope(f"relay#k={k}"):
            to_relay(k).wait_recv()
            g = down if k % 2 else up
            if k == Z:
                ptru[pl.ds(GV * g, GV), :] = ptru[pl.ds(GV * g, GV), :] + rel_t[...]
            else:
                part[:, pl.ds(PAIRS * at(g, zto(k)), PAIRS), :] = take(g, k) + rel[k]
            relayed(k).start()

    def relay_up():
        for k in (Z, *range(0, Z, 2)):
            relay(k)

    def relay_down():
        for k in range(1, Z, 2):
            relay(k)

    inner = (y == 1) | (y == 2)
    pl.when(inner)(relay_up)
    relay_down()
    pl.when(jnp.logical_not(inner))(relay_up)
    with jax.named_scope("known_2"):
        pl.semaphore_wait(known.at[Z2], 2)
        tell(known.at[Y1], beside)
        pl.semaphore_wait(known.at[L1], 3)
        tell(known.at[L2], [other_core])
    direct(Z).wait_recv()
    relayed(Z).wait_recv()
    started(in_m.at[0:4], got.at[DIR_UP]).wait()
    started(in_p.at[0:4], got.at[DIR_DOWN]).wait()
    tsum[...] = ptru[pl.ds(GV * y, GV), :] + (in_mt[...] + in_pt[...])

    def summed(k, out):
        relayed(k).wait_recv()
        x = take(y, k) + (in_m[k] + in_p[k])
        for s in range(4):
            out[PAIRS * s : PAIRS * (s + 1)] = x[s]
        out[4 * PAIRS : ROWS] = tsum[pl.ds((PAIRS * zto(k)) // LEADS, 3), :]

    for k in range(Z - 1):
        with jax.named_scope(f"sum_y#k={k}"):
            summed(k, zout.at[k])
            along_z(k).start()
    summed(Z - 1, sbuf)
    here = lax.broadcasted_iota(jnp.int32, (ROWS, 128), 0) == lax.broadcasted_iota(jnp.int32, (ROWS, 128), 1)
    for k in range(Z):
        x = sbuf[0:ROWS] if k == Z - 1 else zout[k]
        column = jnp.sum(x * wbuf[...], axis=1, keepdims=True)
        lin[lat, pl.ds(zto(k), 1), :] = jnp.sum(jnp.where(here, column, 0.0), axis=0, keepdims=True)

    def to_band(d):
        return remote(lin.at[lat], lin.at[lat], sent.at[0], got.at[L_R], (lax.rem(lat + d, nlat), j))

    def to_all(d):
        return remote(hall.at[j], hall.at[j], sent.at[0], got.at[H_R], (lat, lax.rem(j + d, Y * Z)))

    pl.semaphore_wait(known.at[L2], 1)
    for d in range(1, nlat):
        to_band(d).start()
    s = sbuf[0:ROWS]
    with jax.named_scope("known_3"):
        pl.semaphore_wait(known.at[Y1], 2)
        tell(known.at[Y2], beside)
    with jax.named_scope("sum_z"):
        started(zin, got.at[Z_R]).wait()
        pl.semaphore_wait(known.at[Y2], 2)
    for k in range(Z - 1):
        s = s + zin[k]

    c = 1.0 / NLON
    pair = lax.broadcasted_iota(jnp.int32, (PAIRS, 128), 0) + lax.rem(j, 4)
    sbuf[0:ROWS] = s
    square, offset = sbuf[0:9], sbuf[9:18]
    product, spread = sbuf[18:27], sbuf[27:36]
    truth = jnp.where(pair < 4, sbuf[36:37], jnp.where(pair < 8, sbuf[37:38], sbuf[38:39]))
    mine = pl.ds(PAIRS * j, PAIRS)
    gath[0, mine, :] = square * c
    gath[1, mine, :] = offset * c
    gath[2, mine, :] = (product * c) / jnp.sqrt(jnp.maximum(spread * c, FLOOR) * jnp.maximum(truth * c, FLOOR))

    def scores(owner):
        return gath.at[:, pl.ds(PAIRS * owner, PAIRS), :]

    def spread_z(k, owner):
        return remote(scores(owner), scores(owner), sent.at[0], a_r.at[k], (lat, at(y, zto(k))))

    def along_y(owner):
        for yy in (opposite, up, down):
            remote(scores(owner), scores(owner), sent.at[0], got.at[Y_R], (lat, at(yy, z))).start()

    for k in (0, 1, 2, 3, 4, 5, 6):
        spread_z(k, j).start()
    along_y(j)

    with jax.named_scope("bands"):
        started(prows.at[pl.ds(0, (nlat - 1) * Z)], got.at[L_R]).wait()
    total = lin[0]
    for b in range(1, nlat):
        total = total + lin[b]
    hall[j] = total
    for d in range(1, Y * Z):
        to_all(d).start()

    def from_z(k):
        with jax.named_scope(f"gather_z#k={k}"):
            owner = at(y, zfrom(k))
            spread_z(k, owner).wait_recv()
            along_y(owner)

    near = (6, 5, 3, 4, 1, 2, 0)
    for k in near:
        from_z(k)

    owner = lax.broadcasted_iota(jnp.int32, (Y * Z, 128), 0)
    var = lax.broadcasted_iota(jnp.int32, (Y * Z, 128), 1)
    chosen = []
    for l in range(LEADS):
        mine = lax.shift_right_logical((var * LEADS + l) * 7282, 16)
        chosen.append(jnp.where(mine == owner, 1.0, 0.0).astype(jnp.bfloat16))
    chosen = jnp.concatenate(chosen, axis=1)
    chosen = jnp.concatenate([chosen] * 3, axis=0)
    with jax.named_scope("globals"):
        started(prows.at[pl.ds(0, (Y * Z - 1) * Z)], got.at[H_R]).wait()
    groups = []
    for g in range(Y):
        total = hall[g * Z]
        for zz in range(1, Z):
            total = total + hall[g * Z + zz]
        groups.append(total)
    total = jnp.concatenate(groups, axis=0) * (1.0 / (NLAT * NLON))

    def lane_of(i):
        return jnp.sum(jnp.where(var == i, total, 0.0), axis=1, keepdims=True)

    spread_mean = pltpu.roll(total, 128 - PAIRS, 1)
    pair = var - 2 * PAIRS + lax.rem(owner, 4)
    truth_mean = jnp.where(pair < 4, lane_of(36), jnp.where(pair < 8, lane_of(37), lane_of(38)))
    skill = total / jnp.sqrt(jnp.maximum(spread_mean, FLOOR) * jnp.maximum(truth_mean, FLOOR))
    measures = jnp.where(var < 9, jnp.sqrt(jnp.maximum(total, FLOOR)), jnp.where(var < 18, total, skill))
    table, parts = jnp.where(var < SCORES, measures, 0.0), []
    for _ in range(3):
        parts.append(table.astype(jnp.bfloat16))
        table = table - parts[-1].astype(f32)
    every = lax.dot_general(
        jnp.concatenate(parts, axis=0), chosen, (((0,), (0,)), ((), ())), preferred_element_type=f32
    )
    for l in range(LEADS):
        q = var * LEADS + l
        picked = every[0 : Y * Z, 128 * l : 128 * (l + 1)]
        rest = q - lax.shift_right_logical(q * 7282, 16) * PAIRS
        for m, g in enumerate((g0, g1, g2)):
            line = jnp.sum(jnp.where(owner == rest + m * PAIRS, picked, 0.0), axis=0, keepdims=True)
            g[l : l + 1, :] = line[:, 0:VARS]

    with jax.named_scope("gather_o"):
        started(prows.at[pl.ds(0, 3 * Z * SCORES)], got.at[Y_R]).wait()

    rows = 3 * Z * 4 * PAIRS + 3 * GV + (Z - 1) * ROWS + (4 * Z - 1) * SCORES + (nlat - 1 + Y * Z - 1) * Z
    with jax.named_scope("sends"):
        started(prows.at[pl.ds(0, rows)], sent.at[0]).wait()


def writer(gath, s0, s1, s2, o0, o1, o2, g0, g1, g2, sems):
    rows = LEADS * VARS
    copies = [
        pltpu.make_async_copy(gath.at[m, pl.ds(0, rows)], o.reshape(rows, 128), sems.at[m])
        for m, o in enumerate((o0, o1, o2))
    ]
    copies += [
        pltpu.make_async_copy(s, g, sems.at[3 + m]) for m, (s, g) in enumerate(((s0, g0), (s1, g1), (s2, g2)))
    ]
    for c in copies:
        c.start()
    for c in copies:
        c.wait()


def local(prediction_fields, verifying_state, normal_state, evaluated_point_flag, parallels_each_strip):
    f32 = jnp.float32
    hbm, vmem = pl.BlockSpec(memory_space=pltpu.HBM), pl.BlockSpec(memory_space=pltpu.VMEM)
    dma = pltpu.SemaphoreType.DMA
    single = [jax.ShapeDtypeStruct((LEADS, VARS), f32)] * 3
    gathered, *means = pl.pallas_call(
        kernel,
        out_shape=[jax.ShapeDtypeStruct((3, PADDED, 128), f32)] + single,
        in_specs=[hbm] * 5,
        out_specs=[vmem] * 4,
        scratch_shapes=[
            pltpu.VMEM((TILES, 8, LONS, LEADS, 128), f32),
            pltpu.VMEM((TILES, 2, LONS, 8, 128), f32),
            pltpu.VMEM((LONS, 128), jnp.int32),
            pltpu.SMEM((8,), jnp.int32),
            pltpu.VMEM((LONS, 8, 128), jnp.int32),
            pltpu.VMEM((1, 128), f32),
            pltpu.VMEM((4, PADDED, 128), f32),
            pltpu.VMEM((Y * GV, 128), f32),
            *[pltpu.VMEM((Z, 4, PAIRS, 128), f32), pltpu.VMEM((GV, 128), f32)] * 3,
            pltpu.VMEM((GV, 128), f32),
            pltpu.VMEM((Z - 1, ROWS, 128), f32),
            pltpu.VMEM((Z - 1, ROWS, 128), f32),
            pltpu.VMEM((48, 128), f32),
            pltpu.VMEM((8, Z, 128), f32),
            pltpu.VMEM((Y * Z, Z, 128), f32),
            dma((TILES,)),
            dma((2,)),
            *[dma((Z + 1,))] * 2,
            dma((Z - 1,)),
            dma((1,)),
            dma((8,)),
            pltpu.SemaphoreType.REGULAR((6,)),
        ],
        compiler_params=pltpu.CompilerParams(
            collective_id=0, has_side_effects=True, vmem_limit_bytes=32 * 1024 * 1024
        ),
    )(
        *(
            pltpu.with_memory_space_constraint(x, pltpu.HBM)
            for x in (
                jnp.transpose(prediction_fields, (1, 2, 0, 3)),
                jnp.transpose(verifying_state, (1, 0, 2)),
                jnp.transpose(normal_state, (1, 0, 2)),
                evaluated_point_flag,
                parallels_each_strip,
            )
        )
    )
    *zonal, a, b, c = pl.pallas_call(
        writer,
        out_shape=[jax.ShapeDtypeStruct((VARS, LEADS, 128), f32)] * 3 + single,
        in_specs=[vmem] * 4,
        out_specs=[hbm] * 6,
        scratch_shapes=[dma((6,))],
        compiler_params=pltpu.CompilerParams(vmem_limit_bytes=2 * 1024 * 1024),
    )(gathered, *means)
    return (*(jnp.transpose(o, (1, 0, 2)) for o in zonal), a, b, c)


def solution(mesh):
    placed = (P(None, None, "lon", "lat"), P(None, "lon", "lat"), P(None, "lon", "lat"), P("lon", "lat"), P())
    return jax.shard_map(
        local,
        mesh=mesh,
        in_specs=placed,
        out_specs=(P(None, None, "lat"), P(None, None, "lat"), P(None, None, "lat"), P(), P(), P()),
        check_vma=False,
    )
```
